32 devices in a mesh: beam: 2 (over x), pulse: 16 (over z, y, core).
Axes of the slice: x: 2, y: 2, z: 4, core: 2. Of those that a mesh axis runs over, the one named last changes fastest.
Arguments:
- echoes: float32 [2, 4096, 1536], P(None, 'pulse', 'beam'), parts along dimension 2, may hold values from -6 to 6
- guard_gates: int32 [1], replicated, may hold values from 1 to 4
- train_gates: int32 [1], replicated, may hold values from 4 to 16
Outputs:
- powers: float32 [4096, 1536], P('pulse', 'beam'), parts along dimension 1
- statistic: float32 [4096, 1536], P('pulse', 'beam'), parts along dimension 1
The draws below stay inside these ranges and needn't reach their ends.
There are 2 independent parts, one for each index of `beam`. The reference program is written for one: setup_inputs(seed, part) draws one part's arguments, and reference() takes and returns one part's arrays. A program takes and returns all parts, laid end to end along the dimension named above; an argument that names none is the same for every part. Nothing has to cross between parts.
All inputs are finite; a program needn't handle non-finite values.
Results may differ from the reference program's by a relative error of at most 0.0003.
Values sent between devices are 32-bit elements; how exact they have to be, the bound alone decides.
A program may use at most 192 MiB of HBM per device.

```python
import jax
import jax.numpy as jnp
from jax import lax

PULSES = 4096
GATES = 768
GUARD_BINS = 2
TRAIN_BINS = 4


def block_scale(rng, dims, split, smallest, largest):
    level, own = 1.0, jax.random.fold_in(rng, 6)
    for dim, shards_of in split:
        steps = jnp.exp(jax.random.uniform(jax.random.fold_in(own, dim), (shards_of,), jnp.float32, smallest / len(split), largest / len(split)))
        level = level * jnp.repeat(steps, dims[dim] // shards_of).reshape([-1 if axis == dim else 1 for axis in range(len(dims))])
    return level


def centred(rng, dims, scale, limit, pieces=(), kind=jnp.bfloat16):
    array = jax.random.normal(rng, dims, jnp.float32) * scale
    if len(pieces) > 0:
        array = block_scale(rng, dims, pieces, -0.22, 0.18) * array
    return jnp.clip(array, min=-limit, max=limit).astype(kind)


def setup_inputs(seed: int = 0, part: int = 0) -> dict:
    keys = jax.random.split(jax.random.key(seed), 4)
    part_splits = jax.random.split(jax.random.fold_in(keys[3], part), 4)
    return {
        "echoes": centred(part_splits[0], (2, PULSES, GATES), 1.0, 6.0, ((1, 16),), jnp.float32),
        "guard_gates": jax.random.randint(keys[1], (1,), 1, 5).astype(jnp.int32),
        "train_gates": jax.random.randint(keys[2], (1,), 4, 17).astype(jnp.int32),
    }


TWO_PI = 6.283185307179586

def tables(bin_first, bin_count, pulse_first, pulse_count):
    bin_ids = bin_first + jnp.arange(bin_count, dtype=jnp.int32)
    pulse_ids = pulse_first + jnp.arange(pulse_count, dtype=jnp.int32)
    phases = (bin_ids[:, None] * pulse_ids[None, :] % PULSES).astype(jnp.float32) * (TWO_PI / PULSES)
    return (jnp.cos(phases), jnp.sin(phases))

def transform(cosine, sine, samples):
    width = samples.shape[2]
    stacked = jnp.concatenate([samples[0], samples[1]], axis=1)
    first_part = jnp.dot(cosine, stacked, precision=lax.Precision.HIGHEST, preferred_element_type=jnp.float32)
    second_part = jnp.dot(sine, stacked, precision=lax.Precision.HIGHEST, preferred_element_type=jnp.float32)
    real_part = first_part[:, :width] + second_part[:, width:]
    imag_part = first_part[:, width:] - second_part[:, :width]
    return (real_part, imag_part)

def reference(echoes, guard_gates, train_gates):
    scale_factor = 1.0 / jnp.sqrt(jnp.float32(PULSES))

    def one_block(bin_first):
        cosine, sine = tables(bin_first, 512, 0, PULSES)
        real_part, imag_part = transform(cosine, sine, echoes)
        real_part = real_part * scale_factor
        imag_part = imag_part * scale_factor
        return real_part * real_part + imag_part * imag_part
    starts = jnp.arange(PULSES // 512, dtype=jnp.int32) * 512
    powers = lax.map(one_block, starts).reshape(PULSES, GATES)
    guard_width = guard_gates[0]
    train_width = train_gates[0]
    gate_ids = jnp.arange(GATES, dtype=jnp.int32)
    offsets = jnp.abs(gate_ids[:, None] - gate_ids[None, :])
    band = ((offsets > guard_width) & (offsets <= guard_width + train_width)).astype(jnp.float32)
    range_sum = jnp.dot(powers, band, precision=lax.Precision.HIGHEST, preferred_element_type=jnp.float32)
    range_count = lax.optimization_barrier(jnp.sum(band, axis=0))
    doppler_sum = jnp.zeros_like(powers)
    for shift_bins in range(GUARD_BINS + 1, GUARD_BINS + TRAIN_BINS + 1):
        doppler_sum = doppler_sum + jnp.roll(powers, -shift_bins, axis=0) + jnp.roll(powers, shift_bins, axis=0)
    noise_level = (range_sum + doppler_sum) / (range_count[None, :] + 2.0 * TRAIN_BINS)
    statistic = powers / (noise_level + 1.0)
    return (powers, statistic)
```

```python
import functools

import jax
import jax.numpy as jnp
import numpy as np
from jax import lax
from jax.experimental import pallas as pl
from jax.experimental.pallas import tpu as pltpu
from jax.sharding import PartitionSpec as P

PULSES = 4096
GUARD_BINS = 2
TRAIN_BINS = 4


TWO_PI = 6.283185307179586


def padded_2(cells, sides, width):
    for axis, dim in sides:
        count = lax.axis_size(axis)
        head = lax.slice_in_dim(cells, 0, width, axis=dim)
        tail = lax.slice_in_dim(cells, cells.shape[dim] - width, cells.shape[dim], axis=dim)
        cells = jnp.concatenate(
            [
                lax.ppermute(tail, axis, [(i, (i + 1) % count) for i in range(count)]),
                cells,
                lax.ppermute(head, axis, [((i + 1) % count, i) for i in range(count)]),
            ],
            axis=dim,
        )
    return cells


def small_tables(count):
    index_row = jnp.arange(count, dtype=jnp.int32)
    phases = (index_row[:, None] * index_row[None, :] % count).astype(jnp.float32) * (
        TWO_PI / count
    )
    return (jnp.cos(phases), jnp.sin(phases))


def product(left, right):
    return jnp.dot(left, right, precision=lax.Precision.HIGHEST, preferred_element_type=jnp.float32)


def factored_powers(samples):
    width = samples.shape[2]
    bit_count = PULSES.bit_length() - 1
    first_radix = 2 ** (bit_count // 2)
    second_radix = PULSES // first_radix
    cos_first, sin_first = small_tables(first_radix)
    real_in = samples[0].reshape(first_radix, second_radix * width)
    imag_in = samples[1].reshape(first_radix, second_radix * width)
    real_one = (product(cos_first, real_in) + product(sin_first, imag_in)).reshape(
        first_radix, second_radix, width
    )
    imag_one = (product(cos_first, imag_in) - product(sin_first, real_in)).reshape(
        first_radix, second_radix, width
    )
    first_ids = jnp.arange(first_radix, dtype=jnp.int32)
    second_ids = jnp.arange(second_radix, dtype=jnp.int32)
    twist = (first_ids[:, None] * second_ids[None, :] % PULSES).astype(jnp.float32) * (
        TWO_PI / PULSES
    )
    twist_cos = jnp.cos(twist)[:, :, None]
    twist_sin = jnp.sin(twist)[:, :, None]
    real_two = twist_cos * real_one + twist_sin * imag_one
    imag_two = twist_cos * imag_one - twist_sin * real_one
    real_two = jnp.transpose(real_two, (1, 0, 2)).reshape(second_radix, first_radix * width)
    imag_two = jnp.transpose(imag_two, (1, 0, 2)).reshape(second_radix, first_radix * width)
    cos_second, sin_second = small_tables(second_radix)
    scale_factor = 1.0 / jnp.sqrt(jnp.float32(PULSES))
    real_out = (product(cos_second, real_two) + product(sin_second, imag_two)) * scale_factor
    imag_out = (product(cos_second, imag_two) - product(sin_second, real_two)) * scale_factor
    result = real_out * real_out + imag_out * imag_out
    return result.reshape(PULSES, width)


def generic_shards(echoes, guard_gates, train_gates):
    devices_count = lax.axis_size("pulse")
    bins_local = PULSES // devices_count
    gates_count = echoes.shape[2]
    columns = factored_powers(
        lax.all_to_all(echoes, "pulse", split_axis=2, concat_axis=1, tiled=True)
    )
    powers = lax.all_to_all(columns, "pulse", split_axis=0, concat_axis=1, tiled=True)
    reach = GUARD_BINS + TRAIN_BINS
    padded = padded_2(powers, (("pulse", 0),), reach)
    doppler_sum = jnp.zeros_like(powers)
    for shift_bins in range(GUARD_BINS + 1, reach + 1):
        above = padded[reach + shift_bins : reach + shift_bins + bins_local]
        below = padded[reach - shift_bins : reach - shift_bins + bins_local]
        doppler_sum = doppler_sum + above + below
    guard_width = guard_gates[0]
    train_width = train_gates[0]
    gate_ids = jnp.arange(gates_count, dtype=jnp.int32)
    offsets = jnp.abs(gate_ids[:, None] - gate_ids[None, :])
    band = ((offsets > guard_width) & (offsets <= guard_width + train_width)).astype(jnp.float32)
    range_sum = jnp.dot(
        powers, band, precision=lax.Precision.HIGHEST, preferred_element_type=jnp.float32
    )
    range_count = jnp.sum(band, axis=0)
    noise_level = (range_sum + doppler_sum) / (range_count[None, :] + 2.0 * TRAIN_BINS)
    statistic = powers / (noise_level + 1.0)
    return (powers, statistic)


LANES = 128
ROWS = 8
HIGHEST = lax.Precision.HIGHEST


def butterflies(cells):
    count = len(cells)
    if count == 1:
        return cells
    even = butterflies(cells[0::2])
    odd = butterflies(cells[1::2])
    low, high = [], []
    for k in range(count // 2):
        re, im = odd[k]
        if 4 * k == count:
            re, im = im, -re
        elif k:
            c, s = np.cos(2 * np.pi * k / count), np.sin(2 * np.pi * k / count)
            c, s = np.float32(c), np.float32(s)
            re, im = c * re + s * im, c * im - s * re
        low.append((even[k][0] + re, even[k][1] + im))
        high.append((even[k][0] - re, even[k][1] - im))
    return low + high


def swap_digits(rows, width):
    count = len(rows)
    lane = lax.broadcasted_iota(jnp.int32, rows[0][0].shape, 1)
    bit = 1
    while bit < count:
        step = bit * width
        keep = (lane // step) % 2 == 0 if step < LANES else None
        for f in range(count):
            if f & bit:
                continue
            first, second = rows[f], rows[f | bit]
            if step < LANES:
                new_first = [
                    jnp.where(keep, a, pltpu.roll(b, step, 1)) for a, b in zip(first, second)
                ]
                new_second = [
                    jnp.where(keep, pltpu.roll(a, LANES - step, 1), b)
                    for a, b in zip(first, second)
                ]
            else:
                hop = step // LANES
                new_first, new_second = list(first), list(second)
                for h in range(len(first)):
                    if h & hop:
                        new_first[h] = second[h ^ hop]
                    else:
                        new_second[h] = first[h ^ hop]
            rows[f], rows[f | bit] = new_first, new_second
        bit *= 2
    return rows


def split(values):
    high = values.astype(jnp.bfloat16)
    return high, (values - high.astype(jnp.float32)).astype(jnp.bfloat16)


def bf16_dot(left, right, dims=(((1,), (0,)), ((), ()))):
    return lax.dot_general(left, right, dims, preferred_element_type=jnp.float32)


def inner_flag(me, n):
    plane = lax.div(me, PLANE)
    return lax.rem(lax.div(plane + 1, 2), 2)


def partner(me, offset):
    peer, bit = me, 1
    while bit <= offset:
        if offset & bit:
            peer = peer + bit * (1 - 2 * lax.rem(lax.div(me, bit), 2))
        bit *= 2
    return peer


def peer_orders(n):
    ascending = list(range(1, n))
    if n != PLANES * PLANE:
        return ascending, ascending
    hops = [[plane * PLANE + own for own in range(PLANE)] for plane in range(PLANES)]
    own = hops[0][1:]
    return hops[1] + hops[2] + hops[3] + own, hops[3] + hops[2] + hops[1] + own


def kernel(
    n, chunks, x_any, high_any, low_any, cos_any, sin_any,
    power_ref, total_ref,
    sent, got, mixed, cells, landed, halo_out, halo_in, near_ref,
    x_ref, table_high, table_low, twist_cos, twist_sin,
    send_one, recv_one, send_two, recv_two, send_halo, recv_halo, load, ready,
):
    me = lax.axis_index("pulse")
    length, gates = x_ref.shape[1], x_ref.shape[2]
    wide = gates // chunks
    part = wide // n
    halves = length // LANES
    groups = part // ROWS
    barrier = pltpu.get_barrier_semaphore()
    for k in range(1, n):
        @pl.when(me + k < n)
        def _():
            pl.semaphore_signal(barrier, inc=1, device_id={"pulse": lax.rem(me + k, n)})
    loads = []
    for c in range(chunks):
        for p in range(2):
            lanes = slice(c * wide, (c + 1) * wide)
            loads.append((x_any.at[p, :, lanes], x_ref.at[p, :, lanes]))
    loads += [
        (cos_any, twist_cos), (sin_any, twist_sin), (high_any, table_high), (low_any, table_low),
    ]
    loads = [pltpu.make_async_copy(*pair, load.at[i]) for i, pair in enumerate(loads)]
    for copy in loads:
        copy.start()

    @pl.when(me > 0)
    def _():
        pl.semaphore_wait(barrier, me)

    for k in range(1, n):
        @pl.when(me >= k)
        def _():
            pl.semaphore_signal(
                ready.at[me], inc=1, device_id={"pulse": lax.rem(me + n - k, n)}
            )

    def fill(c):
        for p in range(2):
            loads[2 * c + p].wait()
            block = x_ref[p, :, c * wide : (c + 1) * wide].T
            sent[c, :, p] = block.reshape(n, part, length)

    inner = inner_flag(me, n)
    outer_order, inner_order = peer_orders(n)
    peers = []
    for a, b in zip(outer_order, inner_order):
        if a == b:
            peers.append((a, partner(me, a)))
        else:
            peers.append(
                (
                    a + inner * (b - a),
                    (1 - inner) * partner(me, a) + inner * partner(me, b),
                )
            )

    def first_copy(c, o, peer):
        return pltpu.make_async_remote_copy(
            src_ref=sent.at[c, peer], dst_ref=got.at[c, me],
            send_sem=send_one.at[c, o], recv_sem=recv_one.at[c, o],
            device_id={"pulse": peer},
        )

    def second_copy(c, o, peer):
        return pltpu.make_async_remote_copy(
            src_ref=cells.at[c, peer], dst_ref=landed.at[c, me],
            send_sem=send_two.at[c, o], recv_sem=recv_two.at[c, o],
            device_id={"pulse": peer},
        )

    def halo_copy(c, o, peer):
        return pltpu.make_async_remote_copy(
            src_ref=halo_out.at[c, peer], dst_ref=halo_in.at[c, me],
            send_sem=send_halo.at[c, o], recv_sem=recv_halo.at[c, o],
            device_id={"pulse": peer},
        )

    fill(0)
    for o, peer in peers:
        @pl.when(peer > me)
        def _():
            pl.semaphore_wait(ready.at[peer], 1)

        first_copy(0, o, peer).start()
    for c in range(1, chunks):
        fill(c)
        for o, peer in peers:
            first_copy(c, o, peer).start()
    for c in range(chunks):
        got[c, me] = sent[c, me]
    for copy in loads[2 * chunks :]:
        copy.wait()
    bins = lax.broadcasted_iota(jnp.int32, (length, length), 0)
    bins = jnp.abs(bins - lax.broadcasted_iota(jnp.int32, (length, length), 1))
    inside = (bins > GUARD_BINS) & (bins <= GUARD_BINS + TRAIN_BINS)
    near_ref[...] = inside.astype(jnp.float32).astype(jnp.bfloat16)

    def spectra(c):
        for r in range(0, part, ROWS):
            for h in range(halves):
                lanes = slice(h * LANES, (h + 1) * LANES)
                spectrum = butterflies(
                    [
                        (got[c, s, 0, r : r + ROWS, lanes], got[c, s, 1, r : r + ROWS, lanes])
                        for s in range(n)
                    ]
                )
                for f, (re, im) in enumerate(spectrum):
                    tc, ts = twist_cos[f : f + 1, lanes], twist_sin[f : f + 1, lanes]
                    mixed[0, f, r : r + ROWS, lanes] = tc * re + ts * im
                    mixed[1, f, r : r + ROWS, lanes] = tc * im - ts * re
        high, low = split(mixed[...].reshape(2 * n * part, length))
        both = (
            bf16_dot(high, table_high[...])
            + bf16_dot(low, table_high[...])
            + bf16_dot(high, table_low[...])
        ).reshape(2, n * part, 2 * length)
        real = both[0, :, :length] + both[1, :, length:]
        imag = both[1, :, :length] - both[0, :, length:]
        power = (real * real + imag * imag).reshape(n, part, length)
        rows = [
            [power[f, :, h * LANES : (h + 1) * LANES] for h in range(halves)] for f in range(n)
        ]
        rows = swap_digits(rows, 1)
        lane = lax.broadcasted_iota(jnp.int32, (part, LANES), 1)
        for d in range(n):
            for h in range(halves):
                cells[c, d, :, h * LANES : (h + 1) * LANES] = rows[d][h]
        for d in range(n):
            ends = jnp.where(
                lane >= LANES - ROWS, rows[(d + n - 1) % n][halves - 1],
                jnp.where(lane < ROWS, rows[(d + 1) % n][0], 0.0),
            )
            ends = pltpu.roll(ends, ROWS, 1, stride=2 * ROWS, stride_axis=0)
            halo_out[c, d] = jnp.sum(ends.reshape(groups, ROWS, LANES), axis=1)

    for c in range(chunks):
        for o, peer in peers:
            first_copy(c, o, peer).wait_recv()
        spectra(c)
        for o, peer in peers:
            halo_copy(c, o, peer).start()
            second_copy(c, o, peer).start()
        landed[c, me] = cells[c, me]
        halo_in[c, me] = halo_out[c, me]

    row = lax.broadcasted_iota(jnp.int32, (wide, LANES), 0)
    lane = lax.broadcasted_iota(jnp.int32, (wide, LANES), 1)
    mine = lane // (2 * ROWS) == row % ROWS
    slot = lax.broadcasted_iota(jnp.int32, (2 * ROWS, LANES), 0)
    lane = lax.broadcasted_iota(jnp.int32, (2 * ROWS, LANES), 1)
    fold = (lane % (2 * ROWS) == slot).astype(jnp.float32).astype(jnp.bfloat16)
    rest = jnp.zeros((ROWS, wide), jnp.float32)

    for c in range(chunks):
        for o, peer in peers:
            halo_copy(c, o, peer).wait_recv()
            second_copy(c, o, peer).wait_recv()
        columns = slice(c * wide, (c + 1) * wide)
        powers = landed[c].reshape(wide, length).T
        power_ref[:, columns] = powers
        high, low = split(powers)
        total = bf16_dot(near_ref[...], high) + bf16_dot(near_ref[...], low)
        packed = halo_in[c].reshape(n * groups, 1, LANES)
        packed = jnp.broadcast_to(packed, (n * groups, ROWS, LANES)).reshape(wide, LANES)
        high, low = split(jnp.where(mine, packed, 0.0))
        last_dims = (((1,), (1,)), ((), ()))
        halos = bf16_dot(fold, high, last_dims) + bf16_dot(fold, low, last_dims)
        head = jnp.concatenate([halos[:ROWS], rest])
        tail = jnp.concatenate([rest, halos[ROWS:]])
        top, bottom = total[:ROWS], total[length - ROWS :]
        for d in range(GUARD_BINS + 1, GUARD_BINS + TRAIN_BINS + 1):
            top = top + head[ROWS - d : 2 * ROWS - d]
            bottom = bottom + tail[d : d + ROWS]
        total_ref[:ROWS, columns] = top
        total_ref[ROWS : length - ROWS, columns] = total[ROWS : length - ROWS]
        total_ref[length - ROWS :, columns] = bottom
    for c in range(chunks):
        for o, peer in peers:
            first_copy(c, o, peer).wait_send()
            halo_copy(c, o, peer).wait_send()
            second_copy(c, o, peer).wait_send()


def tables(n, length):
    lane = np.arange(length)
    width = length // n
    bins = width * (lane % n) + lane // n
    turn = 2 * np.pi * (np.outer(lane, bins) % length) / length
    both = np.concatenate([np.cos(turn), np.sin(turn)], axis=1).astype(np.float32)
    high = both.astype(jnp.bfloat16)
    low = (both - high.astype(np.float32)).astype(jnp.bfloat16)
    twist = 2 * np.pi * np.outer(np.arange(n), lane) / (n * length)
    scale = 1.0 / np.sqrt(n * length)
    return (
        high, low,
        (np.cos(twist) * scale).astype(np.float32),
        (np.sin(twist) * scale).astype(np.float32),
    )


def kernel_shards(echoes, guard_gates, train_gates):
    n = lax.axis_size("pulse")
    length, gates = echoes.shape[1], echoes.shape[2]
    chunks = CHUNKS
    part = gates // n // chunks
    wide = n * part
    groups = part // ROWS
    vmem = pl.BlockSpec(memory_space=pltpu.VMEM)
    out = jax.ShapeDtypeStruct((length, gates), jnp.float32)
    dma = pltpu.SemaphoreType.DMA
    operands = (echoes, *(jnp.asarray(t) for t in tables(n, length)))
    results = pl.pallas_call(
        functools.partial(kernel, n, chunks),
        out_shape=(out, out),
        in_specs=[pl.BlockSpec(memory_space=pl.ANY)] * len(operands),
        out_specs=(vmem, vmem),
        scratch_shapes=[
            pltpu.VMEM((chunks, n, 2, part, length), jnp.float32),
            pltpu.VMEM((chunks, n, 2, part, length), jnp.float32),
            pltpu.VMEM((2, n, part, length), jnp.float32),
            pltpu.VMEM((chunks, n, part, length), jnp.float32),
            pltpu.VMEM((chunks, n, part, length), jnp.float32),
            pltpu.VMEM((chunks, n, groups, LANES), jnp.float32),
            pltpu.VMEM((chunks, n, groups, LANES), jnp.float32),
            pltpu.VMEM((length, length), jnp.bfloat16),
            pltpu.VMEM(echoes.shape, jnp.float32),
            pltpu.VMEM((length, 2 * length), jnp.bfloat16),
            pltpu.VMEM((length, 2 * length), jnp.bfloat16),
            pltpu.VMEM((n, length), jnp.float32),
            pltpu.VMEM((n, length), jnp.float32),
            *[dma((chunks, n))] * 6,
            dma((2 * chunks + 4,)),
            pltpu.SemaphoreType.REGULAR((n,)),
        ],
        compiler_params=pltpu.CompilerParams(
            collective_id=0, has_side_effects=True, vmem_limit_bytes=24 * 2**20
        ),
        cost_estimate=pl.CostEstimate(
            flops=KERNEL_FLOPS, bytes_accessed=2 * 4 * length * gates, transcendentals=0
        ),
    )(*(pltpu.with_memory_space_constraint(t, pltpu.HBM) for t in operands))
    return pl.pallas_call(
        write_out,
        out_shape=(out, out),
        in_specs=[vmem] * 4,
        out_specs=(pl.BlockSpec(memory_space=pl.ANY),) * 2,
        scratch_shapes=[pltpu.VMEM((length, gates), jnp.float32), dma((1 + gates // BLOCK,))],
        compiler_params=pltpu.CompilerParams(vmem_limit_bytes=12 * 2**20),
    )(guard_gates, train_gates, *results)


def write_out(guard_ref, train_ref, power_in, total_in, power_out, stat_out, stat_ref, done):
    gates = power_in.shape[1]
    copies = [pltpu.make_async_copy(power_in, power_out, done.at[0])]
    copies[0].start()
    guard, train = guard_ref[...].reshape(1, 1), train_ref[...].reshape(1, 1)
    rows = BLOCK + 2 * LANES
    taps = lax.broadcasted_iota(jnp.int32, (rows, BLOCK), 0) - LANES
    taps = jnp.abs(taps - lax.broadcasted_iota(jnp.int32, (rows, BLOCK), 1))
    inside = (taps > guard) & (taps <= guard + train)
    band = inside.astype(jnp.float32).astype(jnp.bfloat16)
    gate = lax.broadcasted_iota(jnp.int32, (1, gates), 1)
    before = jnp.minimum(jnp.maximum(gate - guard, 0), train)
    after = jnp.minimum(jnp.maximum(gates - 1 - gate - guard, 0), train)
    count = (before + after).astype(jnp.float32) + 2.0 * TRAIN_BINS
    high, low = split(power_in[...])
    for first in range(0, gates, BLOCK):
        last = min(first + BLOCK, gates)
        begin, end = max(0, first - LANES), min(gates, last + LANES)
        taps = band[begin - first + LANES : end - first + LANES, : last - first]
        total = bf16_dot(high[:, begin:end], taps) + bf16_dot(low[:, begin:end], taps)
        scale = count[:, first:last]
        total = total + total_in[:, first:last] + scale
        stat_ref[:, first:last] = power_in[:, first:last] * scale / total
        copies.append(
            pltpu.make_async_copy(
                stat_ref.at[:, first:last], stat_out.at[:, first:last], done.at[len(copies)]
            )
        )
        copies[-1].start()
    for copy in copies:
        copy.wait()


CHUNKS = 2
BLOCK = 256
KERNEL_FLOPS = 10**10
PLANE = 4
PLANES = 4
REACH = 20


def shards(echoes, guard_gates, train_gates):
    n = lax.axis_size("pulse")
    length, gates = echoes.shape[1], echoes.shape[2]
    fits = length % LANES == 0 and length % n == 0 and 2 < n <= LANES
    fits = fits and gates % (n * ROWS * CHUNKS) == 0 and gates % (LANES * CHUNKS) == 0
    fits = fits and n & (n - 1) == 0 and length & (length - 1) == 0 and REACH <= LANES
    if fits and GUARD_BINS + TRAIN_BINS <= ROWS:
        return kernel_shards(echoes, guard_gates, train_gates)
    return generic_shards(echoes, guard_gates, train_gates)


def solution(mesh):
    return jax.shard_map(
        shards,
        mesh=mesh,
        in_specs=(P(None, "pulse", "beam"), P(), P()),
        out_specs=(P("pulse", "beam"), P("pulse", "beam")),
        check_vma=False,
    )
```

```python
import functools

import jax
import jax.numpy as jnp
import numpy as np
from jax import lax
from jax.experimental import pallas as pl
from jax.experimental.pallas import tpu as pltpu
from jax.sharding import PartitionSpec as P

PULSES = 4096
GUARD_BINS = 2
TRAIN_BINS = 4


TWO_PI = 6.283185307179586


def padded_2(cells, sides, width):
    for axis, dim in sides:
        count = lax.axis_size(axis)
        head = lax.slice_in_dim(cells, 0, width, axis=dim)
        tail = lax.slice_in_dim(cells, cells.shape[dim] - width, cells.shape[dim], axis=dim)
        cells = jnp.concatenate(
            [
                lax.ppermute(tail, axis, [(i, (i + 1) % count) for i in range(count)]),
                cells,
                lax.ppermute(head, axis, [((i + 1) % count, i) for i in range(count)]),
            ],
            axis=dim,
        )
    return cells


def small_tables(count):
    index_row = jnp.arange(count, dtype=jnp.int32)
    phases = (index_row[:, None] * index_row[None, :] % count).astype(jnp.float32) * (
        TWO_PI / count
    )
    return (jnp.cos(phases), jnp.sin(phases))


def product(left, right):
    return jnp.dot(left, right, precision=lax.Precision.HIGHEST, preferred_element_type=jnp.float32)


def factored_powers(samples):
    width = samples.shape[2]
    bit_count = PULSES.bit_length() - 1
    first_radix = 2 ** (bit_count // 2)
    second_radix = PULSES // first_radix
    cos_first, sin_first = small_tables(first_radix)
    real_in = samples[0].reshape(first_radix, second_radix * width)
    imag_in = samples[1].reshape(first_radix, second_radix * width)
    real_one = (product(cos_first, real_in) + product(sin_first, imag_in)).reshape(
        first_radix, second_radix, width
    )
    imag_one = (product(cos_first, imag_in) - product(sin_first, real_in)).reshape(
        first_radix, second_radix, width
    )
    first_ids = jnp.arange(first_radix, dtype=jnp.int32)
    second_ids = jnp.arange(second_radix, dtype=jnp.int32)
    twist = (first_ids[:, None] * second_ids[None, :] % PULSES).astype(jnp.float32) * (
        TWO_PI / PULSES
    )
    twist_cos = jnp.cos(twist)[:, :, None]
    twist_sin = jnp.sin(twist)[:, :, None]
    real_two = twist_cos * real_one + twist_sin * imag_one
    imag_two = twist_cos * imag_one - twist_sin * real_one
    real_two = jnp.transpose(real_two, (1, 0, 2)).reshape(second_radix, first_radix * width)
    imag_two = jnp.transpose(imag_two, (1, 0, 2)).reshape(second_radix, first_radix * width)
    cos_second, sin_second = small_tables(second_radix)
    scale_factor = 1.0 / jnp.sqrt(jnp.float32(PULSES))
    real_out = (product(cos_second, real_two) + product(sin_second, imag_two)) * scale_factor
    imag_out = (product(cos_second, imag_two) - product(sin_second, real_two)) * scale_factor
    result = real_out * real_out + imag_out * imag_out
    return result.reshape(PULSES, width)


def generic_shards(echoes, guard_gates, train_gates):
    devices_count = lax.axis_size("pulse")
    bins_local = PULSES // devices_count
    gates_count = echoes.shape[2]
    columns = factored_powers(
        lax.all_to_all(echoes, "pulse", split_axis=2, concat_axis=1, tiled=True)
    )
    powers = lax.all_to_all(columns, "pulse", split_axis=0, concat_axis=1, tiled=True)
    reach = GUARD_BINS + TRAIN_BINS
    padded = padded_2(powers, (("pulse", 0),), reach)
    doppler_sum = jnp.zeros_like(powers)
    for shift_bins in range(GUARD_BINS + 1, reach + 1):
        above = padded[reach + shift_bins : reach + shift_bins + bins_local]
        below = padded[reach - shift_bins : reach - shift_bins + bins_local]
        doppler_sum = doppler_sum + above + below
    guard_width = guard_gates[0]
    train_width = train_gates[0]
    gate_ids = jnp.arange(gates_count, dtype=jnp.int32)
    offsets = jnp.abs(gate_ids[:, None] - gate_ids[None, :])
    band = ((offsets > guard_width) & (offsets <= guard_width + train_width)).astype(jnp.float32)
    range_sum = jnp.dot(
        powers, band, precision=lax.Precision.HIGHEST, preferred_element_type=jnp.float32
    )
    range_count = jnp.sum(band, axis=0)
    noise_level = (range_sum + doppler_sum) / (range_count[None, :] + 2.0 * TRAIN_BINS)
    statistic = powers / (noise_level + 1.0)
    return (powers, statistic)


LANES = 128
ROWS = 8
HIGHEST = lax.Precision.HIGHEST


def butterflies(cells):
    count = len(cells)
    if count == 1:
        return cells
    even = butterflies(cells[0::2])
    odd = butterflies(cells[1::2])
    low, high = [], []
    for k in range(count // 2):
        re, im = odd[k]
        if 4 * k == count:
            re, im = im, -re
        elif k:
            c, s = np.cos(2 * np.pi * k / count), np.sin(2 * np.pi * k / count)
            c, s = np.float32(c), np.float32(s)
            re, im = c * re + s * im, c * im - s * re
        low.append((even[k][0] + re, even[k][1] + im))
        high.append((even[k][0] - re, even[k][1] - im))
    return low + high


def swap_digits(rows, width):
    count = len(rows)
    lane = lax.broadcasted_iota(jnp.int32, rows[0][0].shape, 1)
    bit = 1
    while bit < count:
        step = bit * width
        keep = (lane // step) % 2 == 0 if step < LANES else None
        for f in range(count):
            if f & bit:
                continue
            first, second = rows[f], rows[f | bit]
            if step < LANES:
                new_first = [
                    jnp.where(keep, a, pltpu.roll(b, step, 1)) for a, b in zip(first, second)
                ]
                new_second = [
                    jnp.where(keep, pltpu.roll(a, LANES - step, 1), b)
                    for a, b in zip(first, second)
                ]
            else:
                hop = step // LANES
                new_first, new_second = list(first), list(second)
                for h in range(len(first)):
                    if h & hop:
                        new_first[h] = second[h ^ hop]
                    else:
                        new_second[h] = first[h ^ hop]
            rows[f], rows[f | bit] = new_first, new_second
        bit *= 2
    return rows


def split(values):
    high = values.astype(jnp.bfloat16)
    return high, (values - high.astype(jnp.float32)).astype(jnp.bfloat16)


def bf16_dot(left, right, dims=(((1,), (0,)), ((), ()))):
    return lax.dot_general(left, right, dims, preferred_element_type=jnp.float32)


def inner_flag(me, n):
    plane = lax.div(me, PLANE)
    return lax.rem(lax.div(plane + 1, 2), 2)


def partner(me, offset):
    peer, bit = me, 1
    while bit <= offset:
        if offset & bit:
            peer = peer + bit * (1 - 2 * lax.rem(lax.div(me, bit), 2))
        bit *= 2
    return peer


def peer_orders(n):
    ascending = list(range(1, n))
    if n != PLANES * PLANE:
        return ((ascending, ascending),) * 2
    near, far, across = ([hop * PLANE + own for own in range(PLANE)] for hop in range(1, PLANES))
    own = ascending[: PLANE - 1]
    there = (far + across + near + own, far + across + near + own)
    back = (across + near + far + own, far + across + own + near)
    return there, back


def kernel(
    n, chunks, x_any, guard_any, train_any, high_any, low_any, cos_any, sin_any,
    power_ref, total_ref, scale_ref, band_ref, near_ref,
    sent, got, mixed, cells, landed, halo_out, halo_in, edges,
    x_ref, guard_ref, train_ref, table_high, table_low, twist_cos, twist_sin,
    send_one, recv_one, send_two, recv_two, send_halo, recv_halo, send_edge, recv_edge,
    load, ready,
):
    me = lax.axis_index("pulse")
    length, gates = x_ref.shape[1], x_ref.shape[2]
    wide = gates // chunks
    part = wide // n
    halves = length // LANES
    groups = part // ROWS
    barrier = pltpu.get_barrier_semaphore()
    tiles = wide // LANES
    loads = []
    for t in range(chunks * tiles):
        lanes = slice(t * LANES, (t + 1) * LANES)
        loads.append((x_any.at[:, :, lanes], x_ref.at[:, :, lanes]))
    loads += [
        (guard_any, guard_ref), (train_any, train_ref), (cos_any, twist_cos),
        (sin_any, twist_sin), (high_any, table_high), (low_any, table_low),
    ]
    loads = [pltpu.make_async_copy(*pair, load.at[i]) for i, pair in enumerate(loads)]
    for copy in loads:
        copy.start()
    for k in range(1, n):
        @pl.when(me + k < n)
        def _():
            pl.semaphore_signal(barrier, inc=1, device_id={"pulse": lax.rem(me + k, n)})
    @pl.when(me > 0)
    def _():
        pl.semaphore_wait(barrier, me)

    for k in range(1, n):
        @pl.when(me >= k)
        def _():
            pl.semaphore_signal(
                ready.at[me], inc=1, device_id={"pulse": lax.rem(me + n - k, n)}
            )

    def fill(t):
        loads[t].wait()
        c, first = t // tiles, t % tiles * LANES
        for p in range(2):
            block = x_ref[p, :, t * LANES : (t + 1) * LANES].T
            for d in range(first // part, -(-(first + LANES) // part)):
                begin, end = max(first, d * part), min(first + LANES, (d + 1) * part)
                sent[c, d, p, begin - d * part : end - d * part] = block[begin - first : end - first]

    inner = inner_flag(me, n)
    peers, back = (
        [
            (a + inner * (b - a), (1 - inner) * partner(me, a) + inner * partner(me, b))
            if a != b else (a, partner(me, a))
            for a, b in zip(*orders)
        ]
        for orders in peer_orders(n)
    )

    def first_copy(c, o, peer):
        return pltpu.make_async_remote_copy(
            src_ref=sent.at[c, peer], dst_ref=got.at[c, me],
            send_sem=send_one.at[c, o], recv_sem=recv_one.at[c, o],
            device_id={"pulse": peer},
        )

    def second_copy(c, o, peer):
        return pltpu.make_async_remote_copy(
            src_ref=cells.at[c, peer], dst_ref=landed.at[c, me],
            send_sem=send_two.at[c, o], recv_sem=recv_two.at[c, o],
            device_id={"pulse": peer},
        )

    def halo_copy(o, peer):
        return pltpu.make_async_remote_copy(
            src_ref=halo_out.at[peer], dst_ref=halo_in.at[me],
            send_sem=send_halo.at[o], recv_sem=recv_halo.at[o],
            device_id={"pulse": peer},
        )

    plane, place = lax.div(me, PLANE), lax.rem(me, PLANE)
    below = 0
    for t in range(tiles):
        fill(t)
        covered = (t + 1) * LANES // (part * PLANE)
        for low_plane in range(below, covered):
            @pl.when(plane > low_plane)
            def _():
                for own in range(PLANE):
                    o = partner(plane, low_plane) * PLANE + own
                    first_copy(0, o, low_plane * PLANE + partner(place, own)).start()

        below = covered
    for o, peer in peers:
        @pl.when(lax.div(peer, PLANE) >= plane)
        def _():
            @pl.when(peer > me)
            def _():
                pl.semaphore_wait(ready.at[peer], 1)

            first_copy(0, o, peer).start()

    for c in range(1, chunks):
        for t in range(c * tiles, (c + 1) * tiles):
            fill(t)
        for o, peer in peers:
            first_copy(c, o, peer).start()
    for c in range(chunks):
        got[c, me] = sent[c, me]
    for copy in loads[chunks * tiles :]:
        copy.wait()
    guard, train = guard_ref[0], train_ref[0]
    taps = lax.broadcasted_iota(jnp.int32, band_ref.shape, 0) - LANES
    taps = jnp.abs(taps - lax.broadcasted_iota(jnp.int32, band_ref.shape, 1))
    inside = (taps > guard) & (taps <= guard + train)
    band_ref[...] = inside.astype(jnp.float32).astype(jnp.bfloat16)
    gate = lax.broadcasted_iota(jnp.int32, scale_ref.shape, 1)
    before = jnp.minimum(jnp.maximum(gate - guard, 0), train)
    after = jnp.minimum(jnp.maximum(gates - 1 - gate - guard, 0), train)
    scale_ref[...] = (before + after).astype(jnp.float32) + 2.0 * TRAIN_BINS
    bins = lax.broadcasted_iota(jnp.int32, (length, length), 0)
    bins = jnp.abs(bins - lax.broadcasted_iota(jnp.int32, (length, length), 1))
    inside = (bins > GUARD_BINS) & (bins <= GUARD_BINS + TRAIN_BINS)
    near_ref[...] = inside.astype(jnp.float32).astype(jnp.bfloat16)

    def spectra(c):
        for r in range(0, part, ROWS):
            for h in range(halves):
                lanes = slice(h * LANES, (h + 1) * LANES)
                spectrum = butterflies(
                    [
                        (got[c, s, 0, r : r + ROWS, lanes], got[c, s, 1, r : r + ROWS, lanes])
                        for s in range(n)
                    ]
                )
                for f, (re, im) in enumerate(spectrum):
                    tc, ts = twist_cos[f : f + 1, lanes], twist_sin[f : f + 1, lanes]
                    mixed[0, f, r : r + ROWS, lanes] = tc * re + ts * im
                    mixed[1, f, r : r + ROWS, lanes] = tc * im - ts * re
        high, low = split(mixed[...].reshape(2 * n * part, length))
        both = (
            bf16_dot(high, table_high[...])
            + bf16_dot(low, table_high[...])
            + bf16_dot(high, table_low[...])
        ).reshape(2, n * part, 2 * length)
        real = both[0, :, :length] + both[1, :, length:]
        imag = both[1, :, :length] - both[0, :, length:]
        power = (real * real + imag * imag).reshape(n, part, length)
        rows = [
            [power[f, :, h * LANES : (h + 1) * LANES] for h in range(halves)] for f in range(n)
        ]
        rows = swap_digits(rows, 1)
        for d in range(n):
            for h in range(halves):
                cells[c, d, :, h * LANES : (h + 1) * LANES] = rows[d][h]
        if c < chunks - 1:
            return
        lane = lax.broadcasted_iota(jnp.int32, (part, LANES), 1)
        for d in range(n):
            ends = jnp.where(
                lane >= LANES - ROWS, rows[(d + n - 1) % n][halves - 1],
                jnp.where(lane < ROWS, rows[(d + 1) % n][0], 0.0),
            )
            ends = pltpu.roll(ends, ROWS, 1, stride=2 * ROWS, stride_axis=0)
            halo_out[d] = jnp.sum(ends.reshape(groups, ROWS, LANES), axis=1)

    for c in range(chunks):
        for o, peer in peers:
            first_copy(c, o, peer).wait_recv()
        spectra(c)
        for o, peer in back:
            if c == chunks - 1:
                halo_copy(o, peer).start()
            second_copy(c, o, peer).start()
        landed[c, me] = cells[c, me]
    halo_in[me] = halo_out[me]

    def edge_copies(c):
        ends = ((length - ROWS, 0, 1), (0, 1, n - 1))
        return [
            pltpu.make_async_remote_copy(
                src_ref=power_ref.at[row : row + ROWS, c * wide : (c + 1) * wide],
                dst_ref=edges.at[c, side],
                send_sem=send_edge.at[c, side], recv_sem=recv_edge.at[c, side],
                device_id={"pulse": lax.rem(me + hop, n)},
            )
            for row, side, hop in ends
        ]

    def arrive(c):
        for o, peer in peers:
            second_copy(c, o, peer).wait_recv()
        power_ref[:, c * wide : (c + 1) * wide] = landed[c].reshape(wide, length).T

    rest = jnp.zeros((ROWS, wide), jnp.float32)

    def add_edges(columns, before, after):
        head, tail = jnp.concatenate([before, rest]), jnp.concatenate([rest, after])
        top, bottom = total_ref[:ROWS, columns], total_ref[length - ROWS :, columns]
        for d in range(GUARD_BINS + 1, GUARD_BINS + TRAIN_BINS + 1):
            top = top + head[ROWS - d : 2 * ROWS - d]
            bottom = bottom + tail[d : d + ROWS]
        total_ref[:ROWS, columns] = top
        total_ref[length - ROWS :, columns] = bottom

    final = gates - wide
    for c in range(chunks - 1):
        arrive(c)
        for copy in edge_copies(c):
            copy.start()
    total_ref[:, :final] = scale_ref[:1, :final] + near_sum(near_ref, power_ref[:, :final])
    total_ref[:, final:] = jnp.broadcast_to(scale_ref[:1, final:], (length, wide))
    for first in range(0, gates, BLOCK):
        last, begin = min(first + BLOCK, gates), max(0, first - LANES)
        end = min(final, last + LANES)
        if begin < end:
            total_ref[:, first:last] += band_sum(band_ref, power_ref, first, last, begin, end)
    for c in range(chunks - 1):
        for copy in edge_copies(c):
            copy.wait_recv()
        add_edges(slice(c * wide, (c + 1) * wide), edges[c, 0], edges[c, 1])
    for first in range(0, gates, BLOCK):
        if complete(first, gates, final):
            own = slice(first, min(first + BLOCK, gates))
            total_ref[:, own] = power_ref[:, own] * scale_ref[:1, own] / total_ref[:, own]
    for o, peer in peers:
        halo_copy(o, peer).wait_recv()
    row = lax.broadcasted_iota(jnp.int32, (wide, LANES), 0)
    lane = lax.broadcasted_iota(jnp.int32, (wide, LANES), 1)
    packed = halo_in[...].reshape(n * groups, 1, LANES)
    packed = jnp.broadcast_to(packed, (n * groups, ROWS, LANES)).reshape(wide, LANES)
    high, low = split(jnp.where(lane // (2 * ROWS) == row % ROWS, packed, 0.0))
    slot = lax.broadcasted_iota(jnp.int32, (2 * ROWS, LANES), 0)
    lane = lax.broadcasted_iota(jnp.int32, (2 * ROWS, LANES), 1)
    fold = (lane % (2 * ROWS) == slot).astype(jnp.float32).astype(jnp.bfloat16)
    last_dims = (((1,), (1,)), ((), ()))
    halos = bf16_dot(fold, high, last_dims) + bf16_dot(fold, low, last_dims)
    add_edges(slice(final, gates), halos[:ROWS], halos[ROWS:])
    arrive(chunks - 1)
    for c in range(chunks - 1):
        for copy in edge_copies(c):
            copy.wait_send()
    for o, peer in peers:
        halo_copy(o, peer).wait_send()
    for c in range(chunks):
        for o, peer in peers:
            first_copy(c, o, peer).wait_send()
            second_copy(c, o, peer).wait_send()


def complete(first, gates, final):
    return min(gates, first + BLOCK + LANES) <= final


def near_sum(near_ref, powers):
    high, low = split(powers)
    return bf16_dot(near_ref[...], high) + bf16_dot(near_ref[...], low)


def band_sum(band_ref, power_ref, first, last, begin, end):
    high, low = split(power_ref[:, begin:end])
    band = band_ref[begin - first + LANES : end - first + LANES, : last - first]
    return bf16_dot(high, band) + bf16_dot(low, band)


def tables(n, length):
    lane = np.arange(length)
    width = length // n
    bins = width * (lane % n) + lane // n
    turn = 2 * np.pi * (np.outer(lane, bins) % length) / length
    both = np.concatenate([np.cos(turn), np.sin(turn)], axis=1).astype(np.float32)
    high = both.astype(jnp.bfloat16)
    low = (both - high.astype(np.float32)).astype(jnp.bfloat16)
    twist = 2 * np.pi * np.outer(np.arange(n), lane) / (n * length)
    scale = 1.0 / np.sqrt(n * length)
    return (
        high, low,
        (np.cos(twist) * scale).astype(np.float32),
        (np.sin(twist) * scale).astype(np.float32),
    )


def kernel_shards(echoes, guard_gates, train_gates):
    n = lax.axis_size("pulse")
    length, gates = echoes.shape[1], echoes.shape[2]
    chunks = CHUNKS
    part = gates // n // chunks
    wide = n * part
    groups = part // ROWS
    vmem = pl.BlockSpec(memory_space=pltpu.VMEM)
    out = jax.ShapeDtypeStruct((length, gates), jnp.float32)
    dma = pltpu.SemaphoreType.DMA
    constants = tuple(jnp.asarray(t) for t in tables(n, length))
    echoes, *constants = (
        pltpu.with_memory_space_constraint(t, pltpu.HBM) for t in (echoes, *constants)
    )
    operands = (echoes, guard_gates, train_gates, *constants)
    results = pl.pallas_call(
        functools.partial(kernel, n, chunks),
        out_shape=(
            out, out, jax.ShapeDtypeStruct((ROWS, gates), jnp.float32),
            jax.ShapeDtypeStruct((BLOCK + 2 * LANES, BLOCK), jnp.bfloat16),
            jax.ShapeDtypeStruct((length, length), jnp.bfloat16),
        ),
        in_specs=[pl.BlockSpec(memory_space=pl.ANY)] * len(operands),
        out_specs=(vmem,) * 5,
        scratch_shapes=[
            pltpu.VMEM((chunks, n, 2, part, length), jnp.float32),
            pltpu.VMEM((chunks, n, 2, part, length), jnp.float32),
            pltpu.VMEM((2, n, part, length), jnp.float32),
            pltpu.VMEM((chunks, n, part, length), jnp.float32),
            pltpu.VMEM((chunks, n, part, length), jnp.float32),
            pltpu.VMEM((n, groups, LANES), jnp.float32),
            pltpu.VMEM((n, groups, LANES), jnp.float32),
            pltpu.VMEM((chunks - 1, 2, ROWS, wide), jnp.float32),
            pltpu.VMEM(echoes.shape, jnp.float32),
            pltpu.SMEM((1,), jnp.int32),
            pltpu.SMEM((1,), jnp.int32),
            pltpu.VMEM((length, 2 * length), jnp.bfloat16),
            pltpu.VMEM((length, 2 * length), jnp.bfloat16),
            pltpu.VMEM((n, length), jnp.float32),
            pltpu.VMEM((n, length), jnp.float32),
            *[dma((chunks, n))] * 4, dma((n,)), dma((n,)),
            dma((chunks - 1, 2)), dma((chunks - 1, 2)), dma((gates // LANES + 6,)),
            pltpu.SemaphoreType.REGULAR((n,)),
        ],
        compiler_params=pltpu.CompilerParams(
            collective_id=0, has_side_effects=True, vmem_limit_bytes=24 * 2**20
        ),
        cost_estimate=pl.CostEstimate(
            flops=KERNEL_FLOPS, bytes_accessed=2 * 4 * length * gates, transcendentals=0
        ),
    )(*operands)
    return pl.pallas_call(
        functools.partial(write_out, gates - wide),
        out_shape=(out, out),
        in_specs=[vmem] * 5,
        out_specs=(pl.BlockSpec(memory_space=pl.ANY),) * 2,
        scratch_shapes=[pltpu.VMEM((length, gates), jnp.float32), dma((1 + gates // BLOCK,))],
        compiler_params=pltpu.CompilerParams(vmem_limit_bytes=12 * 2**20),
    )(*results)


def write_out(
    final, power_ref, total_ref, scale_ref, band_ref, near_ref, power_out, stat_out, stat_ref, done
):
    gates = power_ref.shape[1]
    copies = []

    def put(source, target):
        copies.append(pltpu.make_async_copy(source, target, done.at[len(copies)]))
        copies[-1].start()

    put(power_ref, power_out)
    for first in range(0, gates, BLOCK):
        own = slice(first, min(first + BLOCK, gates))
        if complete(first, gates, final):
            put(total_ref.at[:, own], stat_out.at[:, own])
    for first in range(0, gates, BLOCK):
        if complete(first, gates, final):
            continue
        last = min(first + BLOCK, gates)
        begin, end = max(final, first - LANES), min(gates, last + LANES)
        total = total_ref[:, first:last]
        total = total + band_sum(band_ref, power_ref, first, last, begin, end)
        late = max(first, final)
        near = near_sum(near_ref, power_ref[:, late:last])
        if late > first:
            near = jnp.concatenate([jnp.zeros_like(power_ref[:, first:late]), near], axis=1)
        own = slice(first, last)
        stat_ref[:, own] = power_ref[:, own] * scale_ref[:1, own] / (total + near)
        put(stat_ref.at[:, own], stat_out.at[:, own])
    for copy in copies:
        copy.wait()


CHUNKS = 2
BLOCK = 256
KERNEL_FLOPS = 10**10
PLANE = 4
PLANES = 4
REACH = 20


def shards(echoes, guard_gates, train_gates):
    n = lax.axis_size("pulse")
    length, gates = echoes.shape[1], echoes.shape[2]
    fits = length % LANES == 0 and length % n == 0 and 2 < n <= LANES
    fits = fits and gates % (n * ROWS * CHUNKS) == 0 and gates % (LANES * CHUNKS) == 0
    fits = fits and n & (n - 1) == 0 and length & (length - 1) == 0 and REACH <= LANES
    if fits and GUARD_BINS + TRAIN_BINS <= ROWS:
        return kernel_shards(echoes, guard_gates, train_gates)
    return generic_shards(echoes, guard_gates, train_gates)


def solution(mesh):
    return jax.shard_map(
        shards,
        mesh=mesh,
        in_specs=(P(None, "pulse", "beam"), P(), P()),
        out_specs=(P("pulse", "beam"), P("pulse", "beam")),
        check_vma=False,
    )
```

```python
import functools

import jax
import jax.numpy as jnp
import numpy as np
from jax import lax
from jax.experimental import pallas as pl
from jax.experimental.pallas import tpu as pltpu
from jax.sharding import PartitionSpec as P

PULSES = 4096
GUARD_BINS = 2
TRAIN_BINS = 4


TWO_PI = 6.283185307179586


def padded_2(cells, sides, width):
    for axis, dim in sides:
        count = lax.axis_size(axis)
        head = lax.slice_in_dim(cells, 0, width, axis=dim)
        tail = lax.slice_in_dim(cells, cells.shape[dim] - width, cells.shape[dim], axis=dim)
        cells = jnp.concatenate(
            [
                lax.ppermute(tail, axis, [(i, (i + 1) % count) for i in range(count)]),
                cells,
                lax.ppermute(head, axis, [((i + 1) % count, i) for i in range(count)]),
            ],
            axis=dim,
        )
    return cells


def small_tables(count):
    index_row = jnp.arange(count, dtype=jnp.int32)
    phases = (index_row[:, None] * index_row[None, :] % count).astype(jnp.float32) * (
        TWO_PI / count
    )
    return (jnp.cos(phases), jnp.sin(phases))


def product(left, right):
    return jnp.dot(left, right, precision=lax.Precision.HIGHEST, preferred_element_type=jnp.float32)


def factored_powers(samples):
    width = samples.shape[2]
    bit_count = PULSES.bit_length() - 1
    first_radix = 2 ** (bit_count // 2)
    second_radix = PULSES // first_radix
    cos_first, sin_first = small_tables(first_radix)
    real_in = samples[0].reshape(first_radix, second_radix * width)
    imag_in = samples[1].reshape(first_radix, second_radix * width)
    real_one = (product(cos_first, real_in) + product(sin_first, imag_in)).reshape(
        first_radix, second_radix, width
    )
    imag_one = (product(cos_first, imag_in) - product(sin_first, real_in)).reshape(
        first_radix, second_radix, width
    )
    first_ids = jnp.arange(first_radix, dtype=jnp.int32)
    second_ids = jnp.arange(second_radix, dtype=jnp.int32)
    twist = (first_ids[:, None] * second_ids[None, :] % PULSES).astype(jnp.float32) * (
        TWO_PI / PULSES
    )
    twist_cos = jnp.cos(twist)[:, :, None]
    twist_sin = jnp.sin(twist)[:, :, None]
    real_two = twist_cos * real_one + twist_sin * imag_one
    imag_two = twist_cos * imag_one - twist_sin * real_one
    real_two = jnp.transpose(real_two, (1, 0, 2)).reshape(second_radix, first_radix * width)
    imag_two = jnp.transpose(imag_two, (1, 0, 2)).reshape(second_radix, first_radix * width)
    cos_second, sin_second = small_tables(second_radix)
    scale_factor = 1.0 / jnp.sqrt(jnp.float32(PULSES))
    real_out = (product(cos_second, real_two) + product(sin_second, imag_two)) * scale_factor
    imag_out = (product(cos_second, imag_two) - product(sin_second, real_two)) * scale_factor
    result = real_out * real_out + imag_out * imag_out
    return result.reshape(PULSES, width)


def generic_shards(echoes, guard_gates, train_gates):
    devices_count = lax.axis_size("pulse")
    bins_local = PULSES // devices_count
    gates_count = echoes.shape[2]
    columns = factored_powers(
        lax.all_to_all(echoes, "pulse", split_axis=2, concat_axis=1, tiled=True)
    )
    powers = lax.all_to_all(columns, "pulse", split_axis=0, concat_axis=1, tiled=True)
    reach = GUARD_BINS + TRAIN_BINS
    padded = padded_2(powers, (("pulse", 0),), reach)
    doppler_sum = jnp.zeros_like(powers)
    for shift_bins in range(GUARD_BINS + 1, reach + 1):
        above = padded[reach + shift_bins : reach + shift_bins + bins_local]
        below = padded[reach - shift_bins : reach - shift_bins + bins_local]
        doppler_sum = doppler_sum + above + below
    guard_width = guard_gates[0]
    train_width = train_gates[0]
    gate_ids = jnp.arange(gates_count, dtype=jnp.int32)
    offsets = jnp.abs(gate_ids[:, None] - gate_ids[None, :])
    band = ((offsets > guard_width) & (offsets <= guard_width + train_width)).astype(jnp.float32)
    range_sum = jnp.dot(
        powers, band, precision=lax.Precision.HIGHEST, preferred_element_type=jnp.float32
    )
    range_count = jnp.sum(band, axis=0)
    noise_level = (range_sum + doppler_sum) / (range_count[None, :] + 2.0 * TRAIN_BINS)
    statistic = powers / (noise_level + 1.0)
    return (powers, statistic)


LANES = 128
ROWS = 8
HIGHEST = lax.Precision.HIGHEST


def butterflies(cells):
    count = len(cells)
    if count == 1:
        return cells
    even = butterflies(cells[0::2])
    odd = butterflies(cells[1::2])
    low, high = [], []
    for k in range(count // 2):
        re, im = odd[k]
        if 4 * k == count:
            re, im = im, -re
        elif k:
            c, s = np.cos(2 * np.pi * k / count), np.sin(2 * np.pi * k / count)
            c, s = np.float32(c), np.float32(s)
            re, im = c * re + s * im, c * im - s * re
        low.append((even[k][0] + re, even[k][1] + im))
        high.append((even[k][0] - re, even[k][1] - im))
    return low + high


def swap_digits(rows, width):
    count = len(rows)
    lane = lax.broadcasted_iota(jnp.int32, rows[0][0].shape, 1)
    bit = 1
    while bit < count:
        step = bit * width
        keep = (lane // step) % 2 == 0 if step < LANES else None
        for f in range(count):
            if f & bit:
                continue
            first, second = rows[f], rows[f | bit]
            if step < LANES:
                new_first = [
                    jnp.where(keep, a, pltpu.roll(b, step, 1)) for a, b in zip(first, second)
                ]
                new_second = [
                    jnp.where(keep, pltpu.roll(a, LANES - step, 1), b)
                    for a, b in zip(first, second)
                ]
            else:
                hop = step // LANES
                new_first, new_second = list(first), list(second)
                for h in range(len(first)):
                    if h & hop:
                        new_first[h] = second[h ^ hop]
                    else:
                        new_second[h] = first[h ^ hop]
            rows[f], rows[f | bit] = new_first, new_second
        bit *= 2
    return rows


def split(values):
    high = values.astype(jnp.bfloat16)
    return high, (values - high.astype(jnp.float32)).astype(jnp.bfloat16)


def bf16_dot(left, right, dims=(((1,), (0,)), ((), ()))):
    return lax.dot_general(left, right, dims, preferred_element_type=jnp.float32)


def inner_flag(me, n):
    plane = lax.div(me, PLANE)
    return lax.rem(lax.div(plane + 1, 2), 2)


def partner(me, offset):
    peer, bit = me, 1
    while bit <= offset:
        if offset & bit:
            peer = peer + bit * (1 - 2 * lax.rem(lax.div(me, bit), 2))
        bit *= 2
    return peer


def peer_orders(n):
    ascending = list(range(1, n))
    if n != PLANES * PLANE:
        return ((ascending, ascending),) * 2
    near, far, across = ([hop * PLANE + own for own in range(PLANE)] for hop in range(1, PLANES))
    own = ascending[: PLANE - 1]
    there = (far + across + near + own, far + across + near + own)
    back = (across + near + far + own, far + across + own + near)
    return there, back


def kernel(
    n, chunks, x_any, guard_any, train_any, high_any, low_any, cos_any, sin_any,
    power_ref, total_ref, scale_ref, band_ref, near_ref,
    sent, got, mixed, cells, landed, halo_out, halo_in, edges,
    x_ref, guard_ref, train_ref, table_high, table_low, twist_cos, twist_sin,
    send_one, recv_one, send_two, recv_two, send_halo, recv_halo, send_edge, recv_edge,
    load, row_in, last_in, higher, lower, row_known,
):
    me = lax.axis_index("pulse")
    length, gates = x_ref.shape[1], x_ref.shape[2]
    wide = gates // chunks
    part = wide // n
    halves = length // LANES
    groups = part // ROWS
    barrier = pltpu.get_barrier_semaphore()
    tiles = wide // LANES
    loads = []
    for t in range(chunks * tiles):
        lanes = slice(t * LANES, (t + 1) * LANES)
        loads.append((x_any.at[:, :, lanes], x_ref.at[:, :, lanes]))
    loads += [
        (guard_any, guard_ref), (train_any, train_ref), (cos_any, twist_cos),
        (sin_any, twist_sin), (high_any, table_high), (low_any, table_low),
    ]
    loads = [pltpu.make_async_copy(*pair, load.at[i]) for i, pair in enumerate(loads)]
    for copy in loads:
        copy.start()
    planes = n // PLANE
    last_plane = planes - 1
    plane, place = lax.div(me, PLANE), lax.rem(me, PLANE)
    row, core = lax.div(place, CORES), lax.rem(place, CORES)

    def chip(target, other):
        return target * PLANE + (row + other - 2 * other * row) * CORES

    def tell(semaphore, target, other):
        for k in range(CORES):
            peer = chip(target, other) + k
            pl.semaphore_signal(semaphore, inc=1, device_id={"pulse": peer})

    def hear(semaphore):
        pl.semaphore_wait(semaphore, CORES)

    pl.semaphore_signal(barrier, inc=1, device_id={"pulse": partner(me, 1)})

    @pl.when(plane < last_plane)
    def _():
        tell(barrier, plane + 1, 0)

    @pl.when((plane >= 1) & (plane < last_plane))
    def _():
        tell(barrier, plane - 1, 0)

    @pl.when(row == 0)
    def _():
        tell(barrier, plane, 1)

    beneath = lax.div(plane + last_plane, planes)
    above = 1 - lax.div(plane + 2, planes) if planes > 2 else 0
    pl.semaphore_wait(barrier, 1 + CORES * (beneath + above + row))

    @pl.when(row == 1)
    def _():
        tell(row_in, plane, 1)

    @pl.when((plane == last_plane) & (plane >= 1))
    def _():
        tell(last_in, plane - 1, 0)

    @pl.when((plane >= 1) & (plane + 1 < last_plane))
    def _():
        tell(higher.at[2], plane - 1, 0)
        tell(lower.at[2], plane + 1, 0)

    def fill(t):
        loads[t].wait()
        c, first = t // tiles, t % tiles * LANES
        for p in range(2):
            block = x_ref[p, :, t * LANES : (t + 1) * LANES].T
            for d in range(first // part, -(-(first + LANES) // part)):
                begin, end = max(first, d * part), min(first + LANES, (d + 1) * part)
                sent[c, d, p, begin - d * part : end - d * part] = block[begin - first : end - first]

    inner = inner_flag(me, n)
    peers, back = (
        [
            (a + inner * (b - a), (1 - inner) * partner(me, a) + inner * partner(me, b))
            if a != b else (a, partner(me, a))
            for a, b in zip(*orders)
        ]
        for orders in peer_orders(n)
    )

    def first_copy(c, peer, source=me):
        return pltpu.make_async_remote_copy(
            src_ref=sent.at[c, peer], dst_ref=got.at[c, source],
            send_sem=send_one.at[c, peer], recv_sem=recv_one.at[c, source],
            device_id={"pulse": peer},
        )

    def second_copy(c, o, peer):
        return pltpu.make_async_remote_copy(
            src_ref=cells.at[c, peer], dst_ref=landed.at[c, me],
            send_sem=send_two.at[c, o], recv_sem=recv_two.at[c, o],
            device_id={"pulse": peer},
        )

    def halo_copy(o, peer):
        return pltpu.make_async_remote_copy(
            src_ref=halo_out.at[peer], dst_ref=halo_in.at[me],
            send_sem=send_halo.at[o], recv_sem=recv_halo.at[o],
            device_id={"pulse": peer},
        )

    def send(target, other):
        for k in range(CORES):
            first_copy(0, chip(target, other) + partner(core, k)).start()

    for t in range(tiles):
        fill(t)

    @pl.when(plane + 1 < last_plane)
    def _():
        send(plane + 1, 0)

    @pl.when(plane >= 1)
    def _():
        send(plane - 1, 0)

    first_copy(0, partner(me, 1)).start()

    @pl.when((plane >= 2) & (plane < last_plane))
    def _():
        hear(lower.at[2])
        send(plane - 2, 0)

    @pl.when(plane == last_plane - 1)
    def _():
        hear(last_in)

        @pl.when(plane >= 1)
        def _():
            tell(higher.at[2], plane - 1, 0)
            tell(lower.at[2], plane + 1, 0)

        send(plane + 1, 0)

    @pl.when(row == 0)
    def _():
        hear(row_in)

    tell(row_known.at[1], plane, 1)
    hear(row_known.at[1])
    for hop in (1, -1):
        @pl.when((plane + hop >= 0) & (plane + hop <= last_plane))
        def _():
            send(plane + hop, 1)

    send(plane, 1)
    for k in range(2, planes):
        @pl.when(plane + k <= last_plane)
        def _():
            hear(higher.at[k])

        @pl.when((plane >= k) if k > 2 else (plane == last_plane))
        def _():
            hear(lower.at[k])

        if k + 1 < planes:
            @pl.when((plane + k <= last_plane) & (plane >= 1))
            def _():
                tell(higher.at[k + 1], plane - 1, 0)

            @pl.when((plane >= k) & (plane < last_plane))
            def _():
                tell(lower.at[k + 1], plane + 1, 0)

        @pl.when(plane + k <= last_plane)
        def _():
            send(plane + k, 0)

        @pl.when((plane >= k) if k > 2 else (plane == last_plane))
        def _():
            send(plane - k, 0)

        tell(row_known.at[k], plane, 1)
        hear(row_known.at[k])
        for hop in (k, -k):
            @pl.when((plane + hop >= 0) & (plane + hop <= last_plane))
            def _():
                send(plane + hop, 1)

    for c in range(1, chunks):
        for t in range(c * tiles, (c + 1) * tiles):
            fill(t)
        for o, peer in peers:
            first_copy(c, peer).start()
    for c in range(chunks):
        got[c, me] = sent[c, me]
    for copy in loads[chunks * tiles :]:
        copy.wait()
    guard, train = guard_ref[0], train_ref[0]
    taps = lax.broadcasted_iota(jnp.int32, band_ref.shape, 0) - LANES
    taps = jnp.abs(taps - lax.broadcasted_iota(jnp.int32, band_ref.shape, 1))
    inside = (taps > guard) & (taps <= guard + train)
    band_ref[...] = inside.astype(jnp.float32).astype(jnp.bfloat16)
    gate = lax.broadcasted_iota(jnp.int32, scale_ref.shape, 1)
    before = jnp.minimum(jnp.maximum(gate - guard, 0), train)
    after = jnp.minimum(jnp.maximum(gates - 1 - gate - guard, 0), train)
    scale_ref[...] = (before + after).astype(jnp.float32) + 2.0 * TRAIN_BINS
    bins = lax.broadcasted_iota(jnp.int32, (length, length), 0)
    bins = jnp.abs(bins - lax.broadcasted_iota(jnp.int32, (length, length), 1))
    inside = (bins > GUARD_BINS) & (bins <= GUARD_BINS + TRAIN_BINS)
    near_ref[...] = inside.astype(jnp.float32).astype(jnp.bfloat16)

    def spectra(c):
        for r in range(0, part, ROWS):
            for h in range(halves):
                lanes = slice(h * LANES, (h + 1) * LANES)
                spectrum = butterflies(
                    [
                        (got[c, s, 0, r : r + ROWS, lanes], got[c, s, 1, r : r + ROWS, lanes])
                        for s in range(n)
                    ]
                )
                for f, (re, im) in enumerate(spectrum):
                    tc, ts = twist_cos[f : f + 1, lanes], twist_sin[f : f + 1, lanes]
                    mixed[0, f, r : r + ROWS, lanes] = tc * re + ts * im
                    mixed[1, f, r : r + ROWS, lanes] = tc * im - ts * re
        high, low = split(mixed[...].reshape(2 * n * part, length))
        both = (
            bf16_dot(high, table_high[...])
            + bf16_dot(low, table_high[...])
            + bf16_dot(high, table_low[...])
        ).reshape(2, n * part, 2 * length)
        real = both[0, :, :length] + both[1, :, length:]
        imag = both[1, :, :length] - both[0, :, length:]
        power = (real * real + imag * imag).reshape(n, part, length)
        rows = [
            [power[f, :, h * LANES : (h + 1) * LANES] for h in range(halves)] for f in range(n)
        ]
        rows = swap_digits(rows, 1)
        for d in range(n):
            for h in range(halves):
                cells[c, d, :, h * LANES : (h + 1) * LANES] = rows[d][h]
        if c < chunks - 1:
            return
        lane = lax.broadcasted_iota(jnp.int32, (part, LANES), 1)
        for d in range(n):
            ends = jnp.where(
                lane >= LANES - ROWS, rows[(d + n - 1) % n][halves - 1],
                jnp.where(lane < ROWS, rows[(d + 1) % n][0], 0.0),
            )
            ends = pltpu.roll(ends, ROWS, 1, stride=2 * ROWS, stride_axis=0)
            halo_out[d] = jnp.sum(ends.reshape(groups, ROWS, LANES), axis=1)

    for c in range(chunks):
        for o, peer in peers:
            first_copy(c, peer, peer).wait_recv()
        spectra(c)
        for o, peer in back:
            if c == chunks - 1:
                halo_copy(o, peer).start()
            second_copy(c, o, peer).start()
        landed[c, me] = cells[c, me]
    halo_in[me] = halo_out[me]

    def edge_copies(c):
        ends = ((length - ROWS, 0, 1), (0, 1, n - 1))
        return [
            pltpu.make_async_remote_copy(
                src_ref=power_ref.at[row : row + ROWS, c * wide : (c + 1) * wide],
                dst_ref=edges.at[c, side],
                send_sem=send_edge.at[c, side], recv_sem=recv_edge.at[c, side],
                device_id={"pulse": lax.rem(me + hop, n)},
            )
            for row, side, hop in ends
        ]

    def arrive(c):
        for o, peer in peers:
            second_copy(c, o, peer).wait_recv()
        power_ref[:, c * wide : (c + 1) * wide] = landed[c].reshape(wide, length).T

    rest = jnp.zeros((ROWS, wide), jnp.float32)

    def add_edges(columns, before, after):
        head, tail = jnp.concatenate([before, rest]), jnp.concatenate([rest, after])
        top, bottom = total_ref[:ROWS, columns], total_ref[length - ROWS :, columns]
        for d in range(GUARD_BINS + 1, GUARD_BINS + TRAIN_BINS + 1):
            top = top + head[ROWS - d : 2 * ROWS - d]
            bottom = bottom + tail[d : d + ROWS]
        total_ref[:ROWS, columns] = top
        total_ref[length - ROWS :, columns] = bottom

    final = gates - wide
    for c in range(chunks - 1):
        arrive(c)
        for copy in edge_copies(c):
            copy.start()
    total_ref[:, :final] = scale_ref[:1, :final] + near_sum(near_ref, power_ref[:, :final])
    total_ref[:, final:] = jnp.broadcast_to(scale_ref[:1, final:], (length, wide))
    for first in range(0, gates, BLOCK):
        last, begin = min(first + BLOCK, gates), max(0, first - LANES)
        end = min(final, last + LANES)
        if begin < end:
            total_ref[:, first:last] += band_sum(band_ref, power_ref, first, last, begin, end)
    for c in range(chunks - 1):
        for copy in edge_copies(c):
            copy.wait_recv()
        add_edges(slice(c * wide, (c + 1) * wide), edges[c, 0], edges[c, 1])
    for first in range(0, gates, BLOCK):
        if complete(first, gates, final):
            own = slice(first, min(first + BLOCK, gates))
            total_ref[:, own] = power_ref[:, own] * scale_ref[:1, own] / total_ref[:, own]
    for o, peer in peers:
        halo_copy(o, peer).wait_recv()
    gate_row = lax.broadcasted_iota(jnp.int32, (wide, LANES), 0)
    lane = lax.broadcasted_iota(jnp.int32, (wide, LANES), 1)
    packed = halo_in[...].reshape(n * groups, 1, LANES)
    packed = jnp.broadcast_to(packed, (n * groups, ROWS, LANES)).reshape(wide, LANES)
    high, low = split(jnp.where(lane // (2 * ROWS) == gate_row % ROWS, packed, 0.0))
    slot = lax.broadcasted_iota(jnp.int32, (2 * ROWS, LANES), 0)
    lane = lax.broadcasted_iota(jnp.int32, (2 * ROWS, LANES), 1)
    fold = (lane % (2 * ROWS) == slot).astype(jnp.float32).astype(jnp.bfloat16)
    last_dims = (((1,), (1,)), ((), ()))
    halos = bf16_dot(fold, high, last_dims) + bf16_dot(fold, low, last_dims)
    add_edges(slice(final, gates), halos[:ROWS], halos[ROWS:])
    arrive(chunks - 1)
    for c in range(chunks - 1):
        for copy in edge_copies(c):
            copy.wait_send()
    for o, peer in peers:
        halo_copy(o, peer).wait_send()
    for c in range(chunks):
        for o, peer in peers:
            first_copy(c, peer).wait_send()
            second_copy(c, o, peer).wait_send()


def complete(first, gates, final):
    return min(gates, first + BLOCK + LANES) <= final


def near_sum(near_ref, powers):
    high, low = split(powers)
    return bf16_dot(near_ref[...], high) + bf16_dot(near_ref[...], low)


def band_sum(band_ref, power_ref, first, last, begin, end):
    high, low = split(power_ref[:, begin:end])
    band = band_ref[begin - first + LANES : end - first + LANES, : last - first]
    return bf16_dot(high, band) + bf16_dot(low, band)


def tables(n, length):
    lane = np.arange(length)
    width = length // n
    bins = width * (lane % n) + lane // n
    turn = 2 * np.pi * (np.outer(lane, bins) % length) / length
    both = np.concatenate([np.cos(turn), np.sin(turn)], axis=1).astype(np.float32)
    high = both.astype(jnp.bfloat16)
    low = (both - high.astype(np.float32)).astype(jnp.bfloat16)
    twist = 2 * np.pi * np.outer(np.arange(n), lane) / (n * length)
    scale = 1.0 / np.sqrt(n * length)
    return (
        high, low,
        (np.cos(twist) * scale).astype(np.float32),
        (np.sin(twist) * scale).astype(np.float32),
    )


def kernel_shards(echoes, guard_gates, train_gates):
    n = lax.axis_size("pulse")
    length, gates = echoes.shape[1], echoes.shape[2]
    chunks = CHUNKS
    part = gates // n // chunks
    wide = n * part
    groups = part // ROWS
    vmem = pl.BlockSpec(memory_space=pltpu.VMEM)
    out = jax.ShapeDtypeStruct((length, gates), jnp.float32)
    dma = pltpu.SemaphoreType.DMA
    constants = tuple(jnp.asarray(t) for t in tables(n, length))
    echoes, *constants = (
        pltpu.with_memory_space_constraint(t, pltpu.HBM) for t in (echoes, *constants)
    )
    operands = (echoes, guard_gates, train_gates, *constants)
    results = pl.pallas_call(
        functools.partial(kernel, n, chunks),
        out_shape=(
            out, out, jax.ShapeDtypeStruct((ROWS, gates), jnp.float32),
            jax.ShapeDtypeStruct((BLOCK + 2 * LANES, BLOCK), jnp.bfloat16),
            jax.ShapeDtypeStruct((length, length), jnp.bfloat16),
        ),
        in_specs=[pl.BlockSpec(memory_space=pl.ANY)] * len(operands),
        out_specs=(vmem,) * 5,
        scratch_shapes=[
            pltpu.VMEM((chunks, n, 2, part, length), jnp.float32),
            pltpu.VMEM((chunks, n, 2, part, length), jnp.float32),
            pltpu.VMEM((2, n, part, length), jnp.float32),
            pltpu.VMEM((chunks, n, part, length), jnp.float32),
            pltpu.VMEM((chunks, n, part, length), jnp.float32),
            pltpu.VMEM((n, groups, LANES), jnp.float32),
            pltpu.VMEM((n, groups, LANES), jnp.float32),
            pltpu.VMEM((chunks - 1, 2, ROWS, wide), jnp.float32),
            pltpu.VMEM(echoes.shape, jnp.float32),
            pltpu.SMEM((1,), jnp.int32),
            pltpu.SMEM((1,), jnp.int32),
            pltpu.VMEM((length, 2 * length), jnp.bfloat16),
            pltpu.VMEM((length, 2 * length), jnp.bfloat16),
            pltpu.VMEM((n, length), jnp.float32),
            pltpu.VMEM((n, length), jnp.float32),
            *[dma((chunks, n))] * 4, dma((n,)), dma((n,)),
            dma((chunks - 1, 2)), dma((chunks - 1, 2)), dma((gates // LANES + 6,)),
            pltpu.SemaphoreType.REGULAR, pltpu.SemaphoreType.REGULAR,
            *[pltpu.SemaphoreType.REGULAR((max(3, n // PLANE),))] * 3,
        ],
        compiler_params=pltpu.CompilerParams(
            collective_id=0, has_side_effects=True, vmem_limit_bytes=24 * 2**20
        ),
        cost_estimate=pl.CostEstimate(
            flops=KERNEL_FLOPS, bytes_accessed=2 * 4 * length * gates, transcendentals=0
        ),
    )(*operands)
    return pl.pallas_call(
        functools.partial(write_out, gates - wide),
        out_shape=(out, out),
        in_specs=[vmem] * 5,
        out_specs=(pl.BlockSpec(memory_space=pl.ANY),) * 2,
        scratch_shapes=[pltpu.VMEM((length, gates), jnp.float32), dma((1 + gates // BLOCK,))],
        compiler_params=pltpu.CompilerParams(vmem_limit_bytes=12 * 2**20),
    )(*results)


def write_out(
    final, power_ref, total_ref, scale_ref, band_ref, near_ref, power_out, stat_out, stat_ref, done
):
    gates = power_ref.shape[1]
    copies = []

    def put(source, target):
        copies.append(pltpu.make_async_copy(source, target, done.at[len(copies)]))
        copies[-1].start()

    put(power_ref, power_out)
    for first in range(0, gates, BLOCK):
        own = slice(first, min(first + BLOCK, gates))
        if complete(first, gates, final):
            put(total_ref.at[:, own], stat_out.at[:, own])
    for first in range(0, gates, BLOCK):
        if complete(first, gates, final):
            continue
        last = min(first + BLOCK, gates)
        begin, end = max(final, first - LANES), min(gates, last + LANES)
        total = total_ref[:, first:last]
        total = total + band_sum(band_ref, power_ref, first, last, begin, end)
        late = max(first, final)
        near = near_sum(near_ref, power_ref[:, late:last])
        if late > first:
            near = jnp.concatenate([jnp.zeros_like(power_ref[:, first:late]), near], axis=1)
        own = slice(first, last)
        stat_ref[:, own] = power_ref[:, own] * scale_ref[:1, own] / (total + near)
        put(stat_ref.at[:, own], stat_out.at[:, own])
    for copy in copies:
        copy.wait()


CHUNKS = 2
BLOCK = 256
KERNEL_FLOPS = 10**10
PLANE = 4
CORES = 2
PLANES = 4
REACH = 20


def shards(echoes, guard_gates, train_gates):
    n = lax.axis_size("pulse")
    length, gates = echoes.shape[1], echoes.shape[2]
    fits = length % LANES == 0 and length % n == 0 and n % PLANE == 0 and n <= LANES
    fits = fits and gates % (n * ROWS * CHUNKS) == 0 and gates % (LANES * CHUNKS) == 0
    fits = fits and n & (n - 1) == 0 and length & (length - 1) == 0 and REACH <= LANES
    if fits and GUARD_BINS + TRAIN_BINS <= ROWS:
        return kernel_shards(echoes, guard_gates, train_gates)
    return generic_shards(echoes, guard_gates, train_gates)


def solution(mesh):
    return jax.shard_map(
        shards,
        mesh=mesh,
        in_specs=(P(None, "pulse", "beam"), P(), P()),
        out_specs=(P("pulse", "beam"), P("pulse", "beam")),
        check_vma=False,
    )
```

```python
import functools

import jax
import jax.numpy as jnp
import numpy as np
from jax import lax
from jax.experimental import pallas as pl
from jax.experimental.pallas import tpu as pltpu
from jax.sharding import PartitionSpec as P

PULSES = 4096
GUARD_BINS = 2
TRAIN_BINS = 4


TWO_PI = 6.283185307179586


def padded_2(cells, sides, width):
    for axis, dim in sides:
        count = lax.axis_size(axis)
        head = lax.slice_in_dim(cells, 0, width, axis=dim)
        tail = lax.slice_in_dim(cells, cells.shape[dim] - width, cells.shape[dim], axis=dim)
        cells = jnp.concatenate(
            [
                lax.ppermute(tail, axis, [(i, (i + 1) % count) for i in range(count)]),
                cells,
                lax.ppermute(head, axis, [((i + 1) % count, i) for i in range(count)]),
            ],
            axis=dim,
        )
    return cells


def small_tables(count):
    index_row = jnp.arange(count, dtype=jnp.int32)
    phases = (index_row[:, None] * index_row[None, :] % count).astype(jnp.float32) * (
        TWO_PI / count
    )
    return (jnp.cos(phases), jnp.sin(phases))


def product(left, right):
    return jnp.dot(left, right, precision=lax.Precision.HIGHEST, preferred_element_type=jnp.float32)


def factored_powers(samples):
    width = samples.shape[2]
    bit_count = PULSES.bit_length() - 1
    first_radix = 2 ** (bit_count // 2)
    second_radix = PULSES // first_radix
    cos_first, sin_first = small_tables(first_radix)
    real_in = samples[0].reshape(first_radix, second_radix * width)
    imag_in = samples[1].reshape(first_radix, second_radix * width)
    real_one = (product(cos_first, real_in) + product(sin_first, imag_in)).reshape(
        first_radix, second_radix, width
    )
    imag_one = (product(cos_first, imag_in) - product(sin_first, real_in)).reshape(
        first_radix, second_radix, width
    )
    first_ids = jnp.arange(first_radix, dtype=jnp.int32)
    second_ids = jnp.arange(second_radix, dtype=jnp.int32)
    twist = (first_ids[:, None] * second_ids[None, :] % PULSES).astype(jnp.float32) * (
        TWO_PI / PULSES
    )
    twist_cos = jnp.cos(twist)[:, :, None]
    twist_sin = jnp.sin(twist)[:, :, None]
    real_two = twist_cos * real_one + twist_sin * imag_one
    imag_two = twist_cos * imag_one - twist_sin * real_one
    real_two = jnp.transpose(real_two, (1, 0, 2)).reshape(second_radix, first_radix * width)
    imag_two = jnp.transpose(imag_two, (1, 0, 2)).reshape(second_radix, first_radix * width)
    cos_second, sin_second = small_tables(second_radix)
    scale_factor = 1.0 / jnp.sqrt(jnp.float32(PULSES))
    real_out = (product(cos_second, real_two) + product(sin_second, imag_two)) * scale_factor
    imag_out = (product(cos_second, imag_two) - product(sin_second, real_two)) * scale_factor
    result = real_out * real_out + imag_out * imag_out
    return result.reshape(PULSES, width)


def generic_shards(echoes, guard_gates, train_gates):
    devices_count = lax.axis_size("pulse")
    bins_local = PULSES // devices_count
    gates_count = echoes.shape[2]
    columns = factored_powers(
        lax.all_to_all(echoes, "pulse", split_axis=2, concat_axis=1, tiled=True)
    )
    powers = lax.all_to_all(columns, "pulse", split_axis=0, concat_axis=1, tiled=True)
    reach = GUARD_BINS + TRAIN_BINS
    padded = padded_2(powers, (("pulse", 0),), reach)
    doppler_sum = jnp.zeros_like(powers)
    for shift_bins in range(GUARD_BINS + 1, reach + 1):
        above = padded[reach + shift_bins : reach + shift_bins + bins_local]
        below = padded[reach - shift_bins : reach - shift_bins + bins_local]
        doppler_sum = doppler_sum + above + below
    guard_width = guard_gates[0]
    train_width = train_gates[0]
    gate_ids = jnp.arange(gates_count, dtype=jnp.int32)
    offsets = jnp.abs(gate_ids[:, None] - gate_ids[None, :])
    band = ((offsets > guard_width) & (offsets <= guard_width + train_width)).astype(jnp.float32)
    range_sum = jnp.dot(
        powers, band, precision=lax.Precision.HIGHEST, preferred_element_type=jnp.float32
    )
    range_count = jnp.sum(band, axis=0)
    noise_level = (range_sum + doppler_sum) / (range_count[None, :] + 2.0 * TRAIN_BINS)
    statistic = powers / (noise_level + 1.0)
    return (powers, statistic)


LANES = 128
ROWS = 8
HIGHEST = lax.Precision.HIGHEST


def butterflies(cells):
    count = len(cells)
    if count == 1:
        return cells
    even = butterflies(cells[0::2])
    odd = butterflies(cells[1::2])
    low, high = [], []
    for k in range(count // 2):
        re, im = odd[k]
        if 4 * k == count:
            re, im = im, -re
        elif k:
            c, s = np.cos(2 * np.pi * k / count), np.sin(2 * np.pi * k / count)
            c, s = np.float32(c), np.float32(s)
            re, im = c * re + s * im, c * im - s * re
        low.append((even[k][0] + re, even[k][1] + im))
        high.append((even[k][0] - re, even[k][1] - im))
    return low + high


def swap_digits(rows, width):
    count = len(rows)
    lane = lax.broadcasted_iota(jnp.int32, rows[0][0].shape, 1)
    bit = 1
    while bit < count:
        step = bit * width
        keep = (lane // step) % 2 == 0 if step < LANES else None
        for f in range(count):
            if f & bit:
                continue
            first, second = rows[f], rows[f | bit]
            if step < LANES:
                new_first = [
                    jnp.where(keep, a, pltpu.roll(b, step, 1)) for a, b in zip(first, second)
                ]
                new_second = [
                    jnp.where(keep, pltpu.roll(a, LANES - step, 1), b)
                    for a, b in zip(first, second)
                ]
            else:
                hop = step // LANES
                new_first, new_second = list(first), list(second)
                for h in range(len(first)):
                    if h & hop:
                        new_first[h] = second[h ^ hop]
                    else:
                        new_second[h] = first[h ^ hop]
            rows[f], rows[f | bit] = new_first, new_second
        bit *= 2
    return rows


def split(values):
    high = values.astype(jnp.bfloat16)
    return high, (values - high.astype(jnp.float32)).astype(jnp.bfloat16)


def bf16_dot(left, right, dims=(((1,), (0,)), ((), ()))):
    return lax.dot_general(left, right, dims, preferred_element_type=jnp.float32)


def inner_flag(me, n):
    plane = lax.div(me, PLANE)
    return lax.rem(lax.div(plane + 1, 2), 2)


def partner(me, offset):
    peer, bit = me, 1
    while bit <= offset:
        if offset & bit:
            peer = peer + bit * (1 - 2 * lax.rem(lax.div(me, bit), 2))
        bit *= 2
    return peer


def peer_orders(n):
    ascending = list(range(1, n))
    if n != PLANES * PLANE:
        return ((ascending, ascending),) * 2
    near, far, across = ([hop * PLANE + own for own in range(PLANE)] for hop in range(1, PLANES))
    own = ascending[: PLANE - 1]
    there = (near + far + across + own, far + across + near + own)
    near, far, across = near[::-1], far[::-1], across[::-1]
    back = (across + near + far + own, near + far + across + own)
    return there, back


def kernel(
    n, chunks, x_any, guard_any, train_any, high_any, low_any, cos_any, sin_any,
    power_ref, total_ref, scale_ref, band_ref, near_ref,
    sent, got, mixed, cells, landed, halo_out, halo_in, edges,
    x_ref, guard_ref, train_ref, table_high, table_low, twist_cos, twist_sin,
    send_one, recv_one, send_two, recv_two, send_halo, recv_halo, send_edge, recv_edge,
    load, row_in, last_in, higher, lower, row_known,
):
    me = lax.axis_index("pulse")
    length, gates = x_ref.shape[1], x_ref.shape[2]
    wide = gates // chunks
    part = wide // n
    halves = length // LANES
    groups = part // ROWS
    barrier = pltpu.get_barrier_semaphore()
    tiles = wide // LANES
    loads = []
    for t in range(chunks * tiles):
        lanes = slice(t * LANES, (t + 1) * LANES)
        loads.append((x_any.at[:, :, lanes], x_ref.at[:, :, lanes]))
    loads += [
        (guard_any, guard_ref), (train_any, train_ref), (cos_any, twist_cos),
        (sin_any, twist_sin), (high_any, table_high), (low_any, table_low),
    ]
    loads = [pltpu.make_async_copy(*pair, load.at[i]) for i, pair in enumerate(loads)]
    for copy in loads:
        copy.start()
    planes = n // PLANE
    last_plane = planes - 1
    plane, place = lax.div(me, PLANE), lax.rem(me, PLANE)
    row, core = lax.div(place, CORES), lax.rem(place, CORES)

    def chip(target, other):
        return target * PLANE + (row + other - 2 * other * row) * CORES

    def tell(semaphore, target, other):
        for k in range(CORES):
            peer = chip(target, other) + k
            pl.semaphore_signal(semaphore, inc=1, device_id={"pulse": peer})

    def hear(semaphore):
        pl.semaphore_wait(semaphore, CORES)

    pl.semaphore_signal(barrier, inc=1, device_id={"pulse": partner(me, 1)})

    @pl.when(plane < last_plane)
    def _():
        tell(barrier, plane + 1, 0)

    @pl.when((plane >= 1) & (plane < last_plane))
    def _():
        tell(barrier, plane - 1, 0)

    @pl.when(row == 0)
    def _():
        tell(barrier, plane, 1)

    beneath = lax.div(plane + last_plane, planes)
    above = 1 - lax.div(plane + 2, planes) if planes > 2 else 0
    pl.semaphore_wait(barrier, 1 + CORES * (beneath + above + row))

    @pl.when(row == 1)
    def _():
        tell(row_in, plane, 1)

    @pl.when((plane == last_plane) & (plane >= 1))
    def _():
        tell(last_in, plane - 1, 0)

    @pl.when((plane >= 1) & (plane + 1 < last_plane))
    def _():
        tell(higher.at[2], plane - 1, 0)
        tell(lower.at[2], plane + 1, 0)

    def fill(t):
        loads[t].wait()
        c, first = t // tiles, t % tiles * LANES
        for p in range(2):
            block = x_ref[p, :, t * LANES : (t + 1) * LANES].T
            for d in range(first // part, -(-(first + LANES) // part)):
                begin, end = max(first, d * part), min(first + LANES, (d + 1) * part)
                sent[c, d, p, begin - d * part : end - d * part] = block[begin - first : end - first]

    inner = inner_flag(me, n)
    peers, back = (
        [
            (a + inner * (b - a), (1 - inner) * partner(me, a) + inner * partner(me, b))
            if a != b else (a, partner(me, a))
            for a, b in zip(*orders)
        ]
        for orders in peer_orders(n)
    )

    def first_copy(c, peer, source=me):
        return pltpu.make_async_remote_copy(
            src_ref=sent.at[c, peer], dst_ref=got.at[c, source],
            send_sem=send_one.at[c, peer], recv_sem=recv_one.at[c, source],
            device_id={"pulse": peer},
        )

    def second_copy(c, peer, source=me):
        rows = pl.ds(pl.multiple_of(source * part, ROWS), part)
        return pltpu.make_async_remote_copy(
            src_ref=cells.at[c, peer], dst_ref=landed.at[c, rows],
            send_sem=send_two.at[c], recv_sem=recv_two.at[c, source],
            device_id={"pulse": peer},
        )

    def halo_copy(peer):
        return pltpu.make_async_remote_copy(
            src_ref=halo_out.at[peer], dst_ref=halo_in.at[me],
            send_sem=send_halo, recv_sem=recv_halo,
            device_id={"pulse": peer},
        )

    def all_halos():
        others = pl.ds(0, n - 1)
        return pltpu.make_async_remote_copy(
            src_ref=halo_out.at[others], dst_ref=halo_in.at[others],
            send_sem=send_halo, recv_sem=recv_halo, device_id={"pulse": partner(me, 1)},
        )

    def all_sent(c):
        others = cells.at[c, pl.ds(0, n - 1)]
        return pltpu.make_async_remote_copy(
            src_ref=others, dst_ref=others,
            send_sem=send_two.at[c], recv_sem=recv_two.at[c, 0],
            device_id={"pulse": partner(me, 1)},
        )

    def send(target, other):
        for k in range(CORES):
            first_copy(0, chip(target, other) + partner(core, k)).start()

    for t in range(tiles):
        fill(t)

    @pl.when(plane + 1 < last_plane)
    def _():
        send(plane + 1, 0)

    @pl.when(plane >= 1)
    def _():
        send(plane - 1, 0)

    first_copy(0, partner(me, 1)).start()

    @pl.when((plane >= 2) & (plane < last_plane))
    def _():
        hear(lower.at[2])
        send(plane - 2, 0)

    @pl.when(plane == last_plane - 1)
    def _():
        hear(last_in)

        @pl.when(plane >= 1)
        def _():
            tell(higher.at[2], plane - 1, 0)
            tell(lower.at[2], plane + 1, 0)

        send(plane + 1, 0)

    @pl.when(row == 0)
    def _():
        hear(row_in)

    tell(row_known.at[1], plane, 1)
    hear(row_known.at[1])
    for hop in (1, -1):
        @pl.when((plane + hop >= 0) & (plane + hop <= last_plane))
        def _():
            send(plane + hop, 1)

    send(plane, 1)
    for k in range(2, planes):
        @pl.when(plane + k <= last_plane)
        def _():
            hear(higher.at[k])

        @pl.when((plane >= k) if k > 2 else (plane == last_plane))
        def _():
            hear(lower.at[k])

        if k + 1 < planes:
            @pl.when((plane + k <= last_plane) & (plane >= 1))
            def _():
                tell(higher.at[k + 1], plane - 1, 0)

            @pl.when((plane >= k) & (plane < last_plane))
            def _():
                tell(lower.at[k + 1], plane + 1, 0)

        @pl.when(plane + k <= last_plane)
        def _():
            send(plane + k, 0)

        @pl.when((plane >= k) if k > 2 else (plane == last_plane))
        def _():
            send(plane - k, 0)

        tell(row_known.at[k], plane, 1)
        hear(row_known.at[k])
        for hop in (k, -k):
            @pl.when((plane + hop >= 0) & (plane + hop <= last_plane))
            def _():
                send(plane + hop, 1)

    for c in range(1, chunks):
        for t in range(c * tiles, (c + 1) * tiles):
            fill(t)
        for o, peer in peers:
            first_copy(c, peer).start()
    for c in range(chunks):
        got[c, me] = sent[c, me]
    for copy in loads[chunks * tiles :]:
        copy.wait()
    guard, train = guard_ref[0], train_ref[0]
    taps = lax.broadcasted_iota(jnp.int32, band_ref.shape, 0) - LANES
    taps = jnp.abs(taps - lax.broadcasted_iota(jnp.int32, band_ref.shape, 1))
    inside = (taps > guard) & (taps <= guard + train)
    band_ref[...] = inside.astype(jnp.float32).astype(jnp.bfloat16)
    gate = lax.broadcasted_iota(jnp.int32, scale_ref.shape, 1)
    before = jnp.minimum(jnp.maximum(gate - guard, 0), train)
    after = jnp.minimum(jnp.maximum(gates - 1 - gate - guard, 0), train)
    scale_ref[...] = (before + after).astype(jnp.float32) + 2.0 * TRAIN_BINS
    bins = lax.broadcasted_iota(jnp.int32, (length, length), 0)
    bins = jnp.abs(bins - lax.broadcasted_iota(jnp.int32, (length, length), 1))
    inside = (bins > GUARD_BINS) & (bins <= GUARD_BINS + TRAIN_BINS)
    near_ref[...] = inside.astype(jnp.float32).astype(jnp.bfloat16)

    def spectra(c):
        for r in range(0, part, ROWS):
            for h in range(halves):
                lanes = slice(h * LANES, (h + 1) * LANES)
                spectrum = butterflies(
                    [
                        (got[c, s, 0, r : r + ROWS, lanes], got[c, s, 1, r : r + ROWS, lanes])
                        for s in range(n)
                    ]
                )
                for f, (re, im) in enumerate(spectrum):
                    tc, ts = twist_cos[f : f + 1, lanes], twist_sin[f : f + 1, lanes]
                    mixed[0, f, r : r + ROWS, lanes] = tc * re + ts * im
                    mixed[1, f, r : r + ROWS, lanes] = tc * im - ts * re
        high, low = split(mixed[...].reshape(2 * n * part, length))
        both = (
            bf16_dot(high, table_high[...])
            + bf16_dot(low, table_high[...])
            + bf16_dot(high, table_low[...])
        ).reshape(2, n * part, 2 * length)
        real = both[0, :, :length] + both[1, :, length:]
        imag = both[1, :, :length] - both[0, :, length:]
        power = (real * real + imag * imag).reshape(n, part, length)
        rows = [
            [power[f, :, h * LANES : (h + 1) * LANES] for h in range(halves)] for f in range(n)
        ]
        rows = swap_digits(rows, 1)
        for d in range(n):
            for h in range(halves):
                cells[c, d, :, h * LANES : (h + 1) * LANES] = rows[d][h]
        if c < chunks - 1:
            return
        lane = lax.broadcasted_iota(jnp.int32, (part, LANES), 1)
        for d in range(n):
            ends = jnp.where(
                lane >= LANES - ROWS, rows[(d + n - 1) % n][halves - 1],
                jnp.where(lane < ROWS, rows[(d + 1) % n][0], 0.0),
            )
            ends = pltpu.roll(ends, ROWS, 1, stride=2 * ROWS, stride_axis=0)
            halo_out[d] = jnp.sum(ends.reshape(groups, ROWS, LANES), axis=1)

    for c in range(chunks):
        for o, peer in peers:
            first_copy(c, peer, peer).wait_recv()
        spectra(c)
        for o, peer in back:
            if c == chunks - 1:
                halo_copy(peer).start()
            second_copy(c, peer).start()
        landed[c, pl.ds(pl.multiple_of(me * part, ROWS), part)] = cells[c, me]
    halo_in[me] = halo_out[me]

    def edge_copies(c):
        ends = ((length - ROWS, 0, 1), (0, 1, n - 1))
        return [
            pltpu.make_async_remote_copy(
                src_ref=power_ref.at[row : row + ROWS, c * wide : (c + 1) * wide],
                dst_ref=edges.at[c, side],
                send_sem=send_edge.at[c, side], recv_sem=recv_edge.at[c, side],
                device_id={"pulse": lax.rem(me + hop, n)},
            )
            for row, side, hop in ends
        ]

    upper = lax.div(2 * me, n)

    def arrive(c):
        below = 0
        for k in range(tiles):
            covered = -(-(k + 1) * LANES // part)
            for d in range(below, covered):
                peer = d + upper * (n - 1 - 2 * d)

                @pl.when(peer != me)
                def _():
                    second_copy(c, peer, peer).wait_recv()

            below = covered
            first = (k + upper * (tiles - 1 - 2 * k)) * LANES
            rows = pl.ds(pl.multiple_of(first, LANES), LANES)
            columns = pl.ds(pl.multiple_of(c * wide + first, LANES), LANES)
            power_ref[:, columns] = landed[c, rows].T

    rest = jnp.zeros((ROWS, wide), jnp.float32)

    def add_edges(columns, before, after):
        head, tail = jnp.concatenate([before, rest]), jnp.concatenate([rest, after])
        top, bottom = total_ref[:ROWS, columns], total_ref[length - ROWS :, columns]
        for d in range(GUARD_BINS + 1, GUARD_BINS + TRAIN_BINS + 1):
            top = top + head[ROWS - d : 2 * ROWS - d]
            bottom = bottom + tail[d : d + ROWS]
        total_ref[:ROWS, columns] = top
        total_ref[length - ROWS :, columns] = bottom

    final = gates - wide
    for c in range(chunks - 1):
        arrive(c)
        for copy in edge_copies(c):
            copy.start()
    total_ref[:, :final] = scale_ref[:1, :final] + near_sum(near_ref, power_ref[:, :final])
    total_ref[:, final:] = jnp.broadcast_to(scale_ref[:1, final:], (length, wide))
    for first in range(0, gates, BLOCK):
        last, begin = min(first + BLOCK, gates), max(0, first - LANES)
        end = min(final, last + LANES)
        if begin < end:
            total_ref[:, first:last] += band_sum(band_ref, power_ref, first, last, begin, end)
    for c in range(chunks - 1):
        for copy in edge_copies(c):
            copy.wait_recv()
        add_edges(slice(c * wide, (c + 1) * wide), edges[c, 0], edges[c, 1])
    for first in range(0, gates, BLOCK):
        if complete(first, gates, final):
            own = slice(first, min(first + BLOCK, gates))
            total_ref[:, own] = power_ref[:, own] * scale_ref[:1, own] / total_ref[:, own]
    for c in range(chunks):
        for o, peer in peers:
            first_copy(c, peer).wait_send()
        if c < chunks - 1:
            all_sent(c).wait_send()
    for c in range(chunks - 1):
        for copy in edge_copies(c):
            copy.wait_send()
    all_halos().wait_recv()
    gate_row = lax.broadcasted_iota(jnp.int32, (wide, LANES), 0)
    lane = lax.broadcasted_iota(jnp.int32, (wide, LANES), 1)
    packed = halo_in[...].reshape(n * groups, 1, LANES)
    packed = jnp.broadcast_to(packed, (n * groups, ROWS, LANES)).reshape(wide, LANES)
    high, low = split(jnp.where(lane // (2 * ROWS) == gate_row % ROWS, packed, 0.0))
    slot = lax.broadcasted_iota(jnp.int32, (2 * ROWS, LANES), 0)
    lane = lax.broadcasted_iota(jnp.int32, (2 * ROWS, LANES), 1)
    fold = (lane % (2 * ROWS) == slot).astype(jnp.float32).astype(jnp.bfloat16)
    last_dims = (((1,), (1,)), ((), ()))
    halos = bf16_dot(fold, high, last_dims) + bf16_dot(fold, low, last_dims)
    add_edges(slice(final, gates), halos[:ROWS], halos[ROWS:])
    arrive(chunks - 1)
    all_halos().wait_send()
    all_sent(chunks - 1).wait_send()


def complete(first, gates, final):
    return min(gates, first + BLOCK + LANES) <= final


def near_sum(near_ref, powers):
    high, low = split(powers)
    return bf16_dot(near_ref[...], high) + bf16_dot(near_ref[...], low)


def band_sum(band_ref, power_ref, first, last, begin, end):
    high, low = split(power_ref[:, begin:end])
    band = band_ref[begin - first + LANES : end - first + LANES, : last - first]
    return bf16_dot(high, band) + bf16_dot(low, band)


def tables(n, length):
    lane = np.arange(length)
    width = length // n
    bins = width * (lane % n) + lane // n
    turn = 2 * np.pi * (np.outer(lane, bins) % length) / length
    both = np.concatenate([np.cos(turn), np.sin(turn)], axis=1).astype(np.float32)
    high = both.astype(jnp.bfloat16)
    low = (both - high.astype(np.float32)).astype(jnp.bfloat16)
    twist = 2 * np.pi * np.outer(np.arange(n), lane) / (n * length)
    scale = 1.0 / np.sqrt(n * length)
    return (
        high, low,
        (np.cos(twist) * scale).astype(np.float32),
        (np.sin(twist) * scale).astype(np.float32),
    )


def kernel_shards(echoes, guard_gates, train_gates):
    n = lax.axis_size("pulse")
    length, gates = echoes.shape[1], echoes.shape[2]
    chunks = CHUNKS
    part = gates // n // chunks
    wide = n * part
    groups = part // ROWS
    vmem = pl.BlockSpec(memory_space=pltpu.VMEM)
    out = jax.ShapeDtypeStruct((length, gates), jnp.float32)
    dma = pltpu.SemaphoreType.DMA
    constants = tuple(jnp.asarray(t) for t in tables(n, length))
    echoes, *constants = (
        pltpu.with_memory_space_constraint(t, pltpu.HBM) for t in (echoes, *constants)
    )
    operands = (echoes, guard_gates, train_gates, *constants)
    results = pl.pallas_call(
        functools.partial(kernel, n, chunks),
        out_shape=(
            out, out, jax.ShapeDtypeStruct((ROWS, gates), jnp.float32),
            jax.ShapeDtypeStruct((BLOCK + 2 * LANES, BLOCK), jnp.bfloat16),
            jax.ShapeDtypeStruct((length, length), jnp.bfloat16),
        ),
        in_specs=[pl.BlockSpec(memory_space=pl.ANY)] * len(operands),
        out_specs=(vmem,) * 5,
        scratch_shapes=[
            pltpu.VMEM((chunks, n, 2, part, length), jnp.float32),
            pltpu.VMEM((chunks, n, 2, part, length), jnp.float32),
            pltpu.VMEM((2, n, part, length), jnp.float32),
            pltpu.VMEM((chunks, n, part, length), jnp.float32),
            pltpu.VMEM((chunks, wide, length), jnp.float32),
            pltpu.VMEM((n, groups, LANES), jnp.float32),
            pltpu.VMEM((n, groups, LANES), jnp.float32),
            pltpu.VMEM((chunks - 1, 2, ROWS, wide), jnp.float32),
            pltpu.VMEM(echoes.shape, jnp.float32),
            pltpu.SMEM((1,), jnp.int32),
            pltpu.SMEM((1,), jnp.int32),
            pltpu.VMEM((length, 2 * length), jnp.bfloat16),
            pltpu.VMEM((length, 2 * length), jnp.bfloat16),
            pltpu.VMEM((n, length), jnp.float32),
            pltpu.VMEM((n, length), jnp.float32),
            *[dma((chunks, n))] * 2, dma((chunks,)), dma((chunks, n)), dma, dma,
            dma((chunks - 1, 2)), dma((chunks - 1, 2)), dma((gates // LANES + 6,)),
            pltpu.SemaphoreType.REGULAR, pltpu.SemaphoreType.REGULAR,
            *[pltpu.SemaphoreType.REGULAR((max(3, n // PLANE),))] * 3,
        ],
        compiler_params=pltpu.CompilerParams(
            collective_id=0, has_side_effects=True, vmem_limit_bytes=24 * 2**20
        ),
        cost_estimate=pl.CostEstimate(
            flops=KERNEL_FLOPS, bytes_accessed=2 * 4 * length * gates, transcendentals=0
        ),
    )(*operands)
    return pl.pallas_call(
        functools.partial(write_out, gates - wide),
        out_shape=(out, out),
        in_specs=[vmem] * 5,
        out_specs=(pl.BlockSpec(memory_space=pl.ANY),) * 2,
        scratch_shapes=[pltpu.VMEM((length, gates), jnp.float32), dma((1 + gates // BLOCK,))],
        compiler_params=pltpu.CompilerParams(vmem_limit_bytes=12 * 2**20),
    )(*results)


def write_out(
    final, power_ref, total_ref, scale_ref, band_ref, near_ref, power_out, stat_out, stat_ref, done
):
    gates = power_ref.shape[1]
    copies = []

    def put(source, target):
        copies.append(pltpu.make_async_copy(source, target, done.at[len(copies)]))
        copies[-1].start()

    put(power_ref, power_out)
    for first in range(0, gates, BLOCK):
        own = slice(first, min(first + BLOCK, gates))
        if complete(first, gates, final):
            put(total_ref.at[:, own], stat_out.at[:, own])
    for first in range(0, gates, BLOCK):
        if complete(first, gates, final):
            continue
        last = min(first + BLOCK, gates)
        begin, end = max(final, first - LANES), min(gates, last + LANES)
        total = total_ref[:, first:last]
        total = total + band_sum(band_ref, power_ref, first, last, begin, end)
        late = max(first, final)
        near = near_sum(near_ref, power_ref[:, late:last])
        if late > first:
            near = jnp.concatenate([jnp.zeros_like(power_ref[:, first:late]), near], axis=1)
        own = slice(first, last)
        stat_ref[:, own] = power_ref[:, own] * scale_ref[:1, own] / (total + near)
        put(stat_ref.at[:, own], stat_out.at[:, own])
    for copy in copies:
        copy.wait()


CHUNKS = 2
BLOCK = 256
KERNEL_FLOPS = 10**10
PLANE = 4
CORES = 2
PLANES = 4
REACH = 20


def shards(echoes, guard_gates, train_gates):
    n = lax.axis_size("pulse")
    length, gates = echoes.shape[1], echoes.shape[2]
    fits = length % LANES == 0 and length % n == 0 and n % PLANE == 0 and n <= LANES
    fits = fits and gates % (n * ROWS * CHUNKS) == 0 and gates % (LANES * CHUNKS) == 0
    fits = fits and n & (n - 1) == 0 and length & (length - 1) == 0 and REACH <= LANES
    if fits and GUARD_BINS + TRAIN_BINS <= ROWS:
        return kernel_shards(echoes, guard_gates, train_gates)
    return generic_shards(echoes, guard_gates, train_gates)


def solution(mesh):
    return jax.shard_map(
        shards,
        mesh=mesh,
        in_specs=(P(None, "pulse", "beam"), P(), P()),
        out_specs=(P("pulse", "beam"), P("pulse", "beam")),
        check_vma=False,
    )
```

```python
import functools

import jax
import jax.numpy as jnp
import numpy as np
from jax import lax
from jax.experimental import pallas as pl
from jax.experimental.pallas import tpu as pltpu
from jax.sharding import PartitionSpec as P

PULSES = 4096
GUARD_BINS = 2
TRAIN_BINS = 4


TWO_PI = 6.283185307179586


def padded_2(cells, sides, width):
    for axis, dim in sides:
        count = lax.axis_size(axis)
        head = lax.slice_in_dim(cells, 0, width, axis=dim)
        tail = lax.slice_in_dim(cells, cells.shape[dim] - width, cells.shape[dim], axis=dim)
        cells = jnp.concatenate(
            [
                lax.ppermute(tail, axis, [(i, (i + 1) % count) for i in range(count)]),
                cells,
                lax.ppermute(head, axis, [((i + 1) % count, i) for i in range(count)]),
            ],
            axis=dim,
        )
    return cells


def small_tables(count):
    index_row = jnp.arange(count, dtype=jnp.int32)
    phases = (index_row[:, None] * index_row[None, :] % count).astype(jnp.float32) * (
        TWO_PI / count
    )
    return (jnp.cos(phases), jnp.sin(phases))


def product(left, right):
    return jnp.dot(left, right, precision=lax.Precision.HIGHEST, preferred_element_type=jnp.float32)


def factored_powers(samples):
    width = samples.shape[2]
    bit_count = PULSES.bit_length() - 1
    first_radix = 2 ** (bit_count // 2)
    second_radix = PULSES // first_radix
    cos_first, sin_first = small_tables(first_radix)
    real_in = samples[0].reshape(first_radix, second_radix * width)
    imag_in = samples[1].reshape(first_radix, second_radix * width)
    real_one = (product(cos_first, real_in) + product(sin_first, imag_in)).reshape(
        first_radix, second_radix, width
    )
    imag_one = (product(cos_first, imag_in) - product(sin_first, real_in)).reshape(
        first_radix, second_radix, width
    )
    first_ids = jnp.arange(first_radix, dtype=jnp.int32)
    second_ids = jnp.arange(second_radix, dtype=jnp.int32)
    twist = (first_ids[:, None] * second_ids[None, :] % PULSES).astype(jnp.float32) * (
        TWO_PI / PULSES
    )
    twist_cos = jnp.cos(twist)[:, :, None]
    twist_sin = jnp.sin(twist)[:, :, None]
    real_two = twist_cos * real_one + twist_sin * imag_one
    imag_two = twist_cos * imag_one - twist_sin * real_one
    real_two = jnp.transpose(real_two, (1, 0, 2)).reshape(second_radix, first_radix * width)
    imag_two = jnp.transpose(imag_two, (1, 0, 2)).reshape(second_radix, first_radix * width)
    cos_second, sin_second = small_tables(second_radix)
    scale_factor = 1.0 / jnp.sqrt(jnp.float32(PULSES))
    real_out = (product(cos_second, real_two) + product(sin_second, imag_two)) * scale_factor
    imag_out = (product(cos_second, imag_two) - product(sin_second, real_two)) * scale_factor
    result = real_out * real_out + imag_out * imag_out
    return result.reshape(PULSES, width)


def generic_shards(echoes, guard_gates, train_gates):
    devices_count = lax.axis_size("pulse")
    bins_local = PULSES // devices_count
    gates_count = echoes.shape[2]
    columns = factored_powers(
        lax.all_to_all(echoes, "pulse", split_axis=2, concat_axis=1, tiled=True)
    )
    powers = lax.all_to_all(columns, "pulse", split_axis=0, concat_axis=1, tiled=True)
    reach = GUARD_BINS + TRAIN_BINS
    padded = padded_2(powers, (("pulse", 0),), reach)
    doppler_sum = jnp.zeros_like(powers)
    for shift_bins in range(GUARD_BINS + 1, reach + 1):
        above = padded[reach + shift_bins : reach + shift_bins + bins_local]
        below = padded[reach - shift_bins : reach - shift_bins + bins_local]
        doppler_sum = doppler_sum + above + below
    guard_width = guard_gates[0]
    train_width = train_gates[0]
    gate_ids = jnp.arange(gates_count, dtype=jnp.int32)
    offsets = jnp.abs(gate_ids[:, None] - gate_ids[None, :])
    band = ((offsets > guard_width) & (offsets <= guard_width + train_width)).astype(jnp.float32)
    range_sum = jnp.dot(
        powers, band, precision=lax.Precision.HIGHEST, preferred_element_type=jnp.float32
    )
    range_count = jnp.sum(band, axis=0)
    noise_level = (range_sum + doppler_sum) / (range_count[None, :] + 2.0 * TRAIN_BINS)
    statistic = powers / (noise_level + 1.0)
    return (powers, statistic)


LANES = 128
ROWS = 8
HIGHEST = lax.Precision.HIGHEST


def butterflies(cells):
    count = len(cells)
    if count == 1:
        return cells
    even = butterflies(cells[0::2])
    odd = butterflies(cells[1::2])
    low, high = [], []
    for k in range(count // 2):
        re, im = odd[k]
        if 4 * k == count:
            re, im = im, -re
        elif k:
            c, s = np.cos(2 * np.pi * k / count), np.sin(2 * np.pi * k / count)
            c, s = np.float32(c), np.float32(s)
            re, im = c * re + s * im, c * im - s * re
        low.append((even[k][0] + re, even[k][1] + im))
        high.append((even[k][0] - re, even[k][1] - im))
    return low + high


def swap_digits(rows, width):
    count = len(rows)
    lane = lax.broadcasted_iota(jnp.int32, rows[0][0].shape, 1)
    bit = 1
    while bit < count:
        step = bit * width
        keep = (lane // step) % 2 == 0 if step < LANES else None
        for f in range(count):
            if f & bit:
                continue
            first, second = rows[f], rows[f | bit]
            if step < LANES:
                new_first = [
                    jnp.where(keep, a, pltpu.roll(b, step, 1)) for a, b in zip(first, second)
                ]
                new_second = [
                    jnp.where(keep, pltpu.roll(a, LANES - step, 1), b)
                    for a, b in zip(first, second)
                ]
            else:
                hop = step // LANES
                new_first, new_second = list(first), list(second)
                for h in range(len(first)):
                    if h & hop:
                        new_first[h] = second[h ^ hop]
                    else:
                        new_second[h] = first[h ^ hop]
            rows[f], rows[f | bit] = new_first, new_second
        bit *= 2
    return rows


def split(values):
    high = values.astype(jnp.bfloat16)
    return high, (values - high.astype(jnp.float32)).astype(jnp.bfloat16)


def bf16_dot(left, right, dims=(((1,), (0,)), ((), ()))):
    return lax.dot_general(left, right, dims, preferred_element_type=jnp.float32)


def inner_flag(me, n):
    plane = lax.div(me, PLANE)
    return lax.rem(lax.div(plane + 1, 2), 2)


def partner(me, offset):
    peer, bit = me, 1
    while bit <= offset:
        if offset & bit:
            peer = peer + bit * (1 - 2 * lax.rem(lax.div(me, bit), 2))
        bit *= 2
    return peer


def peer_orders(n):
    ascending = list(range(1, n))
    if n != PLANES * PLANE:
        return ((ascending, ascending),) * 2
    near, far, across = ([hop * PLANE + own for own in range(PLANE)] for hop in range(1, PLANES))
    own = ascending[: PLANE - 1]
    there = (near + far + across + own, far + across + near + own)
    near, far, across = near[::-1], far[::-1], across[::-1]
    back = (across + near + far + own, near + far + across + own)
    return there, back


def kernel(
    n, chunks, x_any, guard_any, train_any, high_any, low_any, cos_any, sin_any,
    power_ref, total_ref, scale_ref, band_ref, near_ref,
    sent, got, mixed, cells, landed, halo_out, halo_in, edges,
    x_ref, guard_ref, train_ref, table_high, table_low, twist_cos, twist_sin,
    send_one, recv_one, send_two, recv_two, send_halo, recv_halo, send_edge, recv_edge,
    load, row_in, last_in, higher, lower, row_known,
):
    me = lax.axis_index("pulse")
    length, gates = x_ref.shape[1], x_ref.shape[2]
    wide = gates // chunks
    part = wide // n
    halves = length // LANES
    groups = part // ROWS
    barrier = pltpu.get_barrier_semaphore()
    tiles = wide // LANES
    loads = []
    for t in range(chunks * tiles):
        lanes = slice(t * LANES, (t + 1) * LANES)
        loads.append((x_any.at[:, :, lanes], x_ref.at[:, :, lanes]))
    loads += [
        (guard_any, guard_ref), (train_any, train_ref), (cos_any, twist_cos),
        (sin_any, twist_sin), (high_any, table_high), (low_any, table_low),
    ]
    loads = [pltpu.make_async_copy(*pair, load.at[i]) for i, pair in enumerate(loads)]
    for copy in loads:
        copy.start()
    planes = n // PLANE
    last_plane = planes - 1
    plane, place = lax.div(me, PLANE), lax.rem(me, PLANE)
    row, core = lax.div(place, CORES), lax.rem(place, CORES)

    def chip(target, other):
        return target * PLANE + (row + other - 2 * other * row) * CORES

    def tell(semaphore, target, other):
        for k in range(CORES):
            peer = chip(target, other) + k
            pl.semaphore_signal(semaphore, inc=1, device_id={"pulse": peer})

    def hear(semaphore):
        pl.semaphore_wait(semaphore, CORES)

    pl.semaphore_signal(barrier, inc=1, device_id={"pulse": partner(me, 1)})

    @pl.when(plane < last_plane)
    def _():
        tell(barrier, plane + 1, 0)

    @pl.when((plane >= 1) & (plane < last_plane))
    def _():
        tell(barrier, plane - 1, 0)

    @pl.when(row == 0)
    def _():
        tell(barrier, plane, 1)

    def fill(t):
        loads[t].wait()
        c, first = t // tiles, t % tiles * LANES
        for p in range(2):
            block = x_ref[p, :, t * LANES : (t + 1) * LANES].T
            for d in range(first // part, -(-(first + LANES) // part)):
                begin, end = max(first, d * part), min(first + LANES, (d + 1) * part)
                sent[c, d, p, begin - d * part : end - d * part] = block[begin - first : end - first]

    inner = inner_flag(me, n)
    peers, back = (
        [
            (a + inner * (b - a), (1 - inner) * partner(me, a) + inner * partner(me, b))
            if a != b else (a, partner(me, a))
            for a, b in zip(*orders)
        ]
        for orders in peer_orders(n)
    )

    def first_copy(c, peer, source=me):
        return pltpu.make_async_remote_copy(
            src_ref=sent.at[c, peer], dst_ref=got.at[c, source],
            send_sem=send_one.at[c, peer], recv_sem=recv_one.at[c, source],
            device_id={"pulse": peer},
        )

    def second_copy(c, peer, source=me):
        rows = pl.ds(pl.multiple_of(source * part, ROWS), part)
        return pltpu.make_async_remote_copy(
            src_ref=cells.at[c, peer], dst_ref=landed.at[c, rows],
            send_sem=send_two.at[c], recv_sem=recv_two.at[c, source],
            device_id={"pulse": peer},
        )

    def halo_copy(peer):
        return pltpu.make_async_remote_copy(
            src_ref=halo_out.at[peer], dst_ref=halo_in.at[me],
            send_sem=send_halo, recv_sem=recv_halo,
            device_id={"pulse": peer},
        )

    def all_halos():
        others = pl.ds(0, n - 1)
        return pltpu.make_async_remote_copy(
            src_ref=halo_out.at[others], dst_ref=halo_in.at[others],
            send_sem=send_halo, recv_sem=recv_halo, device_id={"pulse": partner(me, 1)},
        )

    def all_sent(c):
        others = cells.at[c, pl.ds(0, n - 1)]
        return pltpu.make_async_remote_copy(
            src_ref=others, dst_ref=others,
            send_sem=send_two.at[c], recv_sem=recv_two.at[c, 0],
            device_id={"pulse": partner(me, 1)},
        )

    def send(target, other):
        for k in range(CORES):
            first_copy(0, chip(target, other) + partner(core, k)).start()

    for t in range(tiles):
        fill(t)

    beneath = lax.div(plane + last_plane, planes)
    above = 1 - lax.div(plane + 2, planes) if planes > 2 else 0
    pl.semaphore_wait(barrier, 1 + CORES * (beneath + above + row))

    @pl.when(row == 1)
    def _():
        tell(row_in, plane, 1)

    @pl.when((plane == last_plane) & (plane >= 1))
    def _():
        tell(last_in, plane - 1, 0)

    @pl.when((plane >= 1) & (plane + 1 < last_plane))
    def _():
        tell(higher.at[2], plane - 1, 0)
        tell(lower.at[2], plane + 1, 0)

    @pl.when(plane + 1 < last_plane)
    def _():
        send(plane + 1, 0)

    @pl.when(plane >= 1)
    def _():
        send(plane - 1, 0)

    first_copy(0, partner(me, 1)).start()

    @pl.when((plane >= 2) & (plane < last_plane))
    def _():
        hear(lower.at[2])
        send(plane - 2, 0)

    @pl.when(plane == last_plane - 1)
    def _():
        hear(last_in)

        @pl.when(plane >= 1)
        def _():
            tell(higher.at[2], plane - 1, 0)
            tell(lower.at[2], plane + 1, 0)

        send(plane + 1, 0)

    @pl.when(row == 0)
    def _():
        hear(row_in)

    tell(row_known.at[1], plane, 1)
    hear(row_known.at[1])
    for hop in (1, -1):
        @pl.when((plane + hop >= 0) & (plane + hop <= last_plane))
        def _():
            send(plane + hop, 1)

    send(plane, 1)
    for k in range(2, planes):
        @pl.when(plane + k <= last_plane)
        def _():
            hear(higher.at[k])

        @pl.when((plane >= k) if k > 2 else (plane == last_plane))
        def _():
            hear(lower.at[k])

        if k + 1 < planes:
            @pl.when((plane + k <= last_plane) & (plane >= 1))
            def _():
                tell(higher.at[k + 1], plane - 1, 0)

            @pl.when((plane >= k) & (plane < last_plane))
            def _():
                tell(lower.at[k + 1], plane + 1, 0)

        @pl.when(plane + k <= last_plane)
        def _():
            send(plane + k, 0)

        @pl.when((plane >= k) if k > 2 else (plane == last_plane))
        def _():
            send(plane - k, 0)

        tell(row_known.at[k], plane, 1)
        hear(row_known.at[k])
        for hop in (k, -k):
            @pl.when((plane + hop >= 0) & (plane + hop <= last_plane))
            def _():
                send(plane + hop, 1)

    for c in range(1, chunks):
        for t in range(c * tiles, (c + 1) * tiles):
            fill(t)
        for o, peer in peers:
            first_copy(c, peer).start()
    for c in range(chunks):
        got[c, me] = sent[c, me]
    for copy in loads[chunks * tiles :]:
        copy.wait()
    guard, train = guard_ref[0], train_ref[0]
    taps = lax.broadcasted_iota(jnp.int32, band_ref.shape, 0) - LANES
    taps = jnp.abs(taps - lax.broadcasted_iota(jnp.int32, band_ref.shape, 1))
    inside = (taps > guard) & (taps <= guard + train)
    band_ref[...] = inside.astype(jnp.float32).astype(jnp.bfloat16)
    gate = lax.broadcasted_iota(jnp.int32, scale_ref.shape, 1)
    before = jnp.minimum(jnp.maximum(gate - guard, 0), train)
    after = jnp.minimum(jnp.maximum(gates - 1 - gate - guard, 0), train)
    scale_ref[...] = (before + after).astype(jnp.float32) + 2.0 * TRAIN_BINS
    bins = lax.broadcasted_iota(jnp.int32, (length, length), 0)
    bins = jnp.abs(bins - lax.broadcasted_iota(jnp.int32, (length, length), 1))
    inside = (bins > GUARD_BINS) & (bins <= GUARD_BINS + TRAIN_BINS)
    near_ref[...] = inside.astype(jnp.float32).astype(jnp.bfloat16)

    def spectra(c):
        for r in range(0, part, ROWS):
            for h in range(halves):
                lanes = slice(h * LANES, (h + 1) * LANES)
                spectrum = butterflies(
                    [
                        (got[c, s, 0, r : r + ROWS, lanes], got[c, s, 1, r : r + ROWS, lanes])
                        for s in range(n)
                    ]
                )
                for f, (re, im) in enumerate(spectrum):
                    tc, ts = twist_cos[f : f + 1, lanes], twist_sin[f : f + 1, lanes]
                    mixed[0, f, r : r + ROWS, lanes] = tc * re + ts * im
                    mixed[1, f, r : r + ROWS, lanes] = tc * im - ts * re
        high, low = split(mixed[...].reshape(2 * n * part, length))
        both = (
            bf16_dot(high, table_high[...])
            + bf16_dot(low, table_high[...])
            + bf16_dot(high, table_low[...])
        ).reshape(2, n * part, 2 * length)
        real = both[0, :, :length] + both[1, :, length:]
        imag = both[1, :, :length] - both[0, :, length:]
        power = (real * real + imag * imag).reshape(n, part, length)
        rows = [
            [power[f, :, h * LANES : (h + 1) * LANES] for h in range(halves)] for f in range(n)
        ]
        rows = swap_digits(rows, 1)
        for d in range(n):
            for h in range(halves):
                cells[c, d, :, h * LANES : (h + 1) * LANES] = rows[d][h]
        if c < chunks - 1:
            return
        lane = lax.broadcasted_iota(jnp.int32, (part, LANES), 1)
        for d in range(n):
            ends = jnp.where(
                lane >= LANES - ROWS, rows[(d + n - 1) % n][halves - 1],
                jnp.where(lane < ROWS, rows[(d + 1) % n][0], 0.0),
            )
            ends = pltpu.roll(ends, ROWS, 1, stride=2 * ROWS, stride_axis=0)
            halo_out[d] = jnp.sum(ends.reshape(groups, ROWS, LANES), axis=1)

    for c in range(chunks):
        for o, peer in peers:
            first_copy(c, peer, peer).wait_recv()
        spectra(c)
        for o, peer in back:
            if c == chunks - 1:
                halo_copy(peer).start()
            second_copy(c, peer).start()
        landed[c, pl.ds(pl.multiple_of(me * part, ROWS), part)] = cells[c, me]
    halo_in[me] = halo_out[me]

    def edge_copies(c):
        ends = ((length - ROWS, 0, 1), (0, 1, n - 1))
        return [
            pltpu.make_async_remote_copy(
                src_ref=power_ref.at[row : row + ROWS, c * wide : (c + 1) * wide],
                dst_ref=edges.at[c, side],
                send_sem=send_edge.at[c, side], recv_sem=recv_edge.at[c, side],
                device_id={"pulse": lax.rem(me + hop, n)},
            )
            for row, side, hop in ends
        ]

    upper = lax.div(2 * me, n)

    def arrive(c):
        below = 0
        for k in range(tiles):
            covered = -(-(k + 1) * LANES // part)
            for d in range(below, covered):
                peer = d + upper * (n - 1 - 2 * d)

                @pl.when(peer != me)
                def _():
                    second_copy(c, peer, peer).wait_recv()

            below = covered
            first = (k + upper * (tiles - 1 - 2 * k)) * LANES
            rows = pl.ds(pl.multiple_of(first, LANES), LANES)
            columns = pl.ds(pl.multiple_of(c * wide + first, LANES), LANES)
            power_ref[:, columns] = landed[c, rows].T

    rest = jnp.zeros((ROWS, wide), jnp.float32)

    def add_edges(columns, before, after):
        head, tail = jnp.concatenate([before, rest]), jnp.concatenate([rest, after])
        top, bottom = total_ref[:ROWS, columns], total_ref[length - ROWS :, columns]
        for d in range(GUARD_BINS + 1, GUARD_BINS + TRAIN_BINS + 1):
            top = top + head[ROWS - d : 2 * ROWS - d]
            bottom = bottom + tail[d : d + ROWS]
        total_ref[:ROWS, columns] = top
        total_ref[length - ROWS :, columns] = bottom

    final = gates - wide
    for c in range(chunks - 1):
        arrive(c)
        for copy in edge_copies(c):
            copy.start()
    total_ref[:, :final] = scale_ref[:1, :final] + near_sum(near_ref, power_ref[:, :final])
    total_ref[:, final:] = jnp.broadcast_to(scale_ref[:1, final:], (length, wide))
    for first in range(0, gates, BLOCK):
        last, begin = min(first + BLOCK, gates), max(0, first - LANES)
        end = min(final, last + LANES)
        if begin < end:
            total_ref[:, first:last] += band_sum(band_ref, power_ref, first, last, begin, end)
    for c in range(chunks - 1):
        for copy in edge_copies(c):
            copy.wait_recv()
        add_edges(slice(c * wide, (c + 1) * wide), edges[c, 0], edges[c, 1])
    for first in range(0, gates, BLOCK):
        if complete(first, gates, final):
            own = slice(first, min(first + BLOCK, gates))
            total_ref[:, own] = power_ref[:, own] * scale_ref[:1, own] / total_ref[:, own]
    for c in range(chunks):
        for o, peer in peers:
            first_copy(c, peer).wait_send()
        if c < chunks - 1:
            all_sent(c).wait_send()
    for c in range(chunks - 1):
        for copy in edge_copies(c):
            copy.wait_send()
    all_halos().wait_recv()
    gate_row = lax.broadcasted_iota(jnp.int32, (wide, LANES), 0)
    lane = lax.broadcasted_iota(jnp.int32, (wide, LANES), 1)
    packed = halo_in[...].reshape(n * groups, 1, LANES)
    packed = jnp.broadcast_to(packed, (n * groups, ROWS, LANES)).reshape(wide, LANES)
    high, low = split(jnp.where(lane // (2 * ROWS) == gate_row % ROWS, packed, 0.0))
    slot = lax.broadcasted_iota(jnp.int32, (2 * ROWS, LANES), 0)
    lane = lax.broadcasted_iota(jnp.int32, (2 * ROWS, LANES), 1)
    fold = (lane % (2 * ROWS) == slot).astype(jnp.float32).astype(jnp.bfloat16)
    last_dims = (((1,), (1,)), ((), ()))
    halos = bf16_dot(fold, high, last_dims) + bf16_dot(fold, low, last_dims)
    add_edges(slice(final, gates), halos[:ROWS], halos[ROWS:])
    arrive(chunks - 1)
    all_halos().wait_send()
    all_sent(chunks - 1).wait_send()


def complete(first, gates, final):
    return min(gates, first + BLOCK + LANES) <= final


def near_sum(near_ref, powers):
    high, low = split(powers)
    return bf16_dot(near_ref[...], high) + bf16_dot(near_ref[...], low)


def band_sum(band_ref, power_ref, first, last, begin, end):
    high, low = split(power_ref[:, begin:end])
    band = band_ref[begin - first + LANES : end - first + LANES, : last - first]
    return bf16_dot(high, band) + bf16_dot(low, band)


def tables(n, length):
    lane = np.arange(length)
    width = length // n
    bins = width * (lane % n) + lane // n
    turn = 2 * np.pi * (np.outer(lane, bins) % length) / length
    both = np.concatenate([np.cos(turn), np.sin(turn)], axis=1).astype(np.float32)
    high = both.astype(jnp.bfloat16)
    low = (both - high.astype(np.float32)).astype(jnp.bfloat16)
    twist = 2 * np.pi * np.outer(np.arange(n), lane) / (n * length)
    scale = 1.0 / np.sqrt(n * length)
    return (
        high, low,
        (np.cos(twist) * scale).astype(np.float32),
        (np.sin(twist) * scale).astype(np.float32),
    )


def kernel_shards(echoes, guard_gates, train_gates):
    n = lax.axis_size("pulse")
    length, gates = echoes.shape[1], echoes.shape[2]
    chunks = CHUNKS
    part = gates // n // chunks
    wide = n * part
    groups = part // ROWS
    vmem = pl.BlockSpec(memory_space=pltpu.VMEM)
    out = jax.ShapeDtypeStruct((length, gates), jnp.float32)
    dma = pltpu.SemaphoreType.DMA
    constants = tuple(jnp.asarray(t) for t in tables(n, length))
    echoes, *constants = (
        pltpu.with_memory_space_constraint(t, pltpu.HBM) for t in (echoes, *constants)
    )
    operands = (echoes, guard_gates, train_gates, *constants)
    results = pl.pallas_call(
        functools.partial(kernel, n, chunks),
        out_shape=(
            out, out, jax.ShapeDtypeStruct((ROWS, gates), jnp.float32),
            jax.ShapeDtypeStruct((BLOCK + 2 * LANES, BLOCK), jnp.bfloat16),
            jax.ShapeDtypeStruct((length, length), jnp.bfloat16),
        ),
        in_specs=[pl.BlockSpec(memory_space=pl.ANY)] * len(operands),
        out_specs=(vmem,) * 5,
        scratch_shapes=[
            pltpu.VMEM((chunks, n, 2, part, length), jnp.float32),
            pltpu.VMEM((chunks, n, 2, part, length), jnp.float32),
            pltpu.VMEM((2, n, part, length), jnp.float32),
            pltpu.VMEM((chunks, n, part, length), jnp.float32),
            pltpu.VMEM((chunks, wide, length), jnp.float32),
            pltpu.VMEM((n, groups, LANES), jnp.float32),
            pltpu.VMEM((n, groups, LANES), jnp.float32),
            pltpu.VMEM((chunks - 1, 2, ROWS, wide), jnp.float32),
            pltpu.VMEM(echoes.shape, jnp.float32),
            pltpu.SMEM((1,), jnp.int32),
            pltpu.SMEM((1,), jnp.int32),
            pltpu.VMEM((length, 2 * length), jnp.bfloat16),
            pltpu.VMEM((length, 2 * length), jnp.bfloat16),
            pltpu.VMEM((n, length), jnp.float32),
            pltpu.VMEM((n, length), jnp.float32),
            *[dma((chunks, n))] * 2, dma((chunks,)), dma((chunks, n)), dma, dma,
            dma((chunks - 1, 2)), dma((chunks - 1, 2)), dma((gates // LANES + 6,)),
            pltpu.SemaphoreType.REGULAR, pltpu.SemaphoreType.REGULAR,
            *[pltpu.SemaphoreType.REGULAR((max(3, n // PLANE),))] * 3,
        ],
        compiler_params=pltpu.CompilerParams(
            collective_id=0, has_side_effects=True, vmem_limit_bytes=24 * 2**20
        ),
        cost_estimate=pl.CostEstimate(
            flops=KERNEL_FLOPS, bytes_accessed=2 * 4 * length * gates, transcendentals=0
        ),
    )(*operands)
    return pl.pallas_call(
        functools.partial(write_out, gates - wide),
        out_shape=(out, out),
        in_specs=[vmem] * 5,
        out_specs=(pl.BlockSpec(memory_space=pl.ANY),) * 2,
        scratch_shapes=[pltpu.VMEM((length, gates), jnp.float32), dma((1 + gates // BLOCK,))],
        compiler_params=pltpu.CompilerParams(vmem_limit_bytes=12 * 2**20),
    )(*results)


def write_out(
    final, power_ref, total_ref, scale_ref, band_ref, near_ref, power_out, stat_out, stat_ref, done
):
    gates = power_ref.shape[1]
    copies = []

    def put(source, target):
        copies.append(pltpu.make_async_copy(source, target, done.at[len(copies)]))
        copies[-1].start()

    put(power_ref, power_out)
    for first in range(0, gates, BLOCK):
        own = slice(first, min(first + BLOCK, gates))
        if complete(first, gates, final):
            put(total_ref.at[:, own], stat_out.at[:, own])
    for first in range(0, gates, BLOCK):
        if complete(first, gates, final):
            continue
        last = min(first + BLOCK, gates)
        begin, end = max(final, first - LANES), min(gates, last + LANES)
        total = total_ref[:, first:last]
        total = total + band_sum(band_ref, power_ref, first, last, begin, end)
        late = max(first, final)
        near = near_sum(near_ref, power_ref[:, late:last])
        if late > first:
            near = jnp.concatenate([jnp.zeros_like(power_ref[:, first:late]), near], axis=1)
        own = slice(first, last)
        stat_ref[:, own] = power_ref[:, own] * scale_ref[:1, own] / (total + near)
        put(stat_ref.at[:, own], stat_out.at[:, own])
    for copy in copies:
        copy.wait()


CHUNKS = 2
BLOCK = 256
KERNEL_FLOPS = 10**10
PLANE = 4
CORES = 2
PLANES = 4
REACH = 20


def shards(echoes, guard_gates, train_gates):
    n = lax.axis_size("pulse")
    length, gates = echoes.shape[1], echoes.shape[2]
    fits = length % LANES == 0 and length % n == 0 and n % PLANE == 0 and n <= LANES
    fits = fits and gates % (n * ROWS * CHUNKS) == 0 and gates % (LANES * CHUNKS) == 0
    fits = fits and n & (n - 1) == 0 and length & (length - 1) == 0 and REACH <= LANES
    if fits and GUARD_BINS + TRAIN_BINS <= ROWS:
        return kernel_shards(echoes, guard_gates, train_gates)
    return generic_shards(echoes, guard_gates, train_gates)


def solution(mesh):
    return jax.shard_map(
        shards,
        mesh=mesh,
        in_specs=(P(None, "pulse", "beam"), P(), P()),
        out_specs=(P("pulse", "beam"), P("pulse", "beam")),
        check_vma=False,
    )
```

```python
import functools

import jax
import jax.numpy as jnp
import numpy as np
from jax import lax
from jax.experimental import pallas as pl
from jax.experimental.pallas import tpu as pltpu
from jax.sharding import PartitionSpec as P

PULSES = 4096
GUARD_BINS = 2
TRAIN_BINS = 4


TWO_PI = 6.283185307179586


def padded_2(cells, sides, width):
    for axis, dim in sides:
        count = lax.axis_size(axis)
        head = lax.slice_in_dim(cells, 0, width, axis=dim)
        tail = lax.slice_in_dim(cells, cells.shape[dim] - width, cells.shape[dim], axis=dim)
        cells = jnp.concatenate(
            [
                lax.ppermute(tail, axis, [(i, (i + 1) % count) for i in range(count)]),
                cells,
                lax.ppermute(head, axis, [((i + 1) % count, i) for i in range(count)]),
            ],
            axis=dim,
        )
    return cells


def small_tables(count):
    index_row = jnp.arange(count, dtype=jnp.int32)
    phases = (index_row[:, None] * index_row[None, :] % count).astype(jnp.float32) * (
        TWO_PI / count
    )
    return (jnp.cos(phases), jnp.sin(phases))


def product(left, right):
    return jnp.dot(left, right, precision=lax.Precision.HIGHEST, preferred_element_type=jnp.float32)


def factored_powers(samples):
    width = samples.shape[2]
    bit_count = PULSES.bit_length() - 1
    first_radix = 2 ** (bit_count // 2)
    second_radix = PULSES // first_radix
    cos_first, sin_first = small_tables(first_radix)
    real_in = samples[0].reshape(first_radix, second_radix * width)
    imag_in = samples[1].reshape(first_radix, second_radix * width)
    real_one = (product(cos_first, real_in) + product(sin_first, imag_in)).reshape(
        first_radix, second_radix, width
    )
    imag_one = (product(cos_first, imag_in) - product(sin_first, real_in)).reshape(
        first_radix, second_radix, width
    )
    first_ids = jnp.arange(first_radix, dtype=jnp.int32)
    second_ids = jnp.arange(second_radix, dtype=jnp.int32)
    twist = (first_ids[:, None] * second_ids[None, :] % PULSES).astype(jnp.float32) * (
        TWO_PI / PULSES
    )
    twist_cos = jnp.cos(twist)[:, :, None]
    twist_sin = jnp.sin(twist)[:, :, None]
    real_two = twist_cos * real_one + twist_sin * imag_one
    imag_two = twist_cos * imag_one - twist_sin * real_one
    real_two = jnp.transpose(real_two, (1, 0, 2)).reshape(second_radix, first_radix * width)
    imag_two = jnp.transpose(imag_two, (1, 0, 2)).reshape(second_radix, first_radix * width)
    cos_second, sin_second = small_tables(second_radix)
    scale_factor = 1.0 / jnp.sqrt(jnp.float32(PULSES))
    real_out = (product(cos_second, real_two) + product(sin_second, imag_two)) * scale_factor
    imag_out = (product(cos_second, imag_two) - product(sin_second, real_two)) * scale_factor
    result = real_out * real_out + imag_out * imag_out
    return result.reshape(PULSES, width)


def generic_shards(echoes, guard_gates, train_gates):
    devices_count = lax.axis_size("pulse")
    bins_local = PULSES // devices_count
    gates_count = echoes.shape[2]
    columns = factored_powers(
        lax.all_to_all(echoes, "pulse", split_axis=2, concat_axis=1, tiled=True)
    )
    powers = lax.all_to_all(columns, "pulse", split_axis=0, concat_axis=1, tiled=True)
    reach = GUARD_BINS + TRAIN_BINS
    padded = padded_2(powers, (("pulse", 0),), reach)
    doppler_sum = jnp.zeros_like(powers)
    for shift_bins in range(GUARD_BINS + 1, reach + 1):
        above = padded[reach + shift_bins : reach + shift_bins + bins_local]
        below = padded[reach - shift_bins : reach - shift_bins + bins_local]
        doppler_sum = doppler_sum + above + below
    guard_width = guard_gates[0]
    train_width = train_gates[0]
    gate_ids = jnp.arange(gates_count, dtype=jnp.int32)
    offsets = jnp.abs(gate_ids[:, None] - gate_ids[None, :])
    band = ((offsets > guard_width) & (offsets <= guard_width + train_width)).astype(jnp.float32)
    range_sum = jnp.dot(
        powers, band, precision=lax.Precision.HIGHEST, preferred_element_type=jnp.float32
    )
    range_count = jnp.sum(band, axis=0)
    noise_level = (range_sum + doppler_sum) / (range_count[None, :] + 2.0 * TRAIN_BINS)
    statistic = powers / (noise_level + 1.0)
    return (powers, statistic)


LANES = 128
ROWS = 8
HIGHEST = lax.Precision.HIGHEST


def butterflies(cells):
    count = len(cells)
    if count == 1:
        return cells
    even = butterflies(cells[0::2])
    odd = butterflies(cells[1::2])
    low, high = [], []
    for k in range(count // 2):
        re, im = odd[k]
        if 4 * k == count:
            re, im = im, -re
        elif k:
            c, s = np.cos(2 * np.pi * k / count), np.sin(2 * np.pi * k / count)
            c, s = np.float32(c), np.float32(s)
            re, im = c * re + s * im, c * im - s * re
        low.append((even[k][0] + re, even[k][1] + im))
        high.append((even[k][0] - re, even[k][1] - im))
    return low + high


def swap_digits(rows, width):
    count = len(rows)
    lane = lax.broadcasted_iota(jnp.int32, rows[0][0].shape, 1)
    bit = 1
    while bit < count:
        step = bit * width
        keep = (lane // step) % 2 == 0 if step < LANES else None
        for f in range(count):
            if f & bit:
                continue
            first, second = rows[f], rows[f | bit]
            if step < LANES:
                new_first = [
                    jnp.where(keep, a, pltpu.roll(b, step, 1)) for a, b in zip(first, second)
                ]
                new_second = [
                    jnp.where(keep, pltpu.roll(a, LANES - step, 1), b)
                    for a, b in zip(first, second)
                ]
            else:
                hop = step // LANES
                new_first, new_second = list(first), list(second)
                for h in range(len(first)):
                    if h & hop:
                        new_first[h] = second[h ^ hop]
                    else:
                        new_second[h] = first[h ^ hop]
            rows[f], rows[f | bit] = new_first, new_second
        bit *= 2
    return rows


def split(values):
    high = values.astype(jnp.bfloat16)
    return high, (values - high.astype(jnp.float32)).astype(jnp.bfloat16)


def bf16_dot(left, right, dims=(((1,), (0,)), ((), ()))):
    return lax.dot_general(left, right, dims, preferred_element_type=jnp.float32)


def inner_flag(me, n):
    plane = lax.div(me, PLANE)
    return lax.rem(lax.div(plane + 1, 2), 2)


def partner(me, offset):
    peer, bit = me, 1
    while bit <= offset:
        if offset & bit:
            peer = peer + bit * (1 - 2 * lax.rem(lax.div(me, bit), 2))
        bit *= 2
    return peer


def peer_orders(n):
    ascending = list(range(1, n))
    if n != PLANES * PLANE:
        return ((ascending, ascending),) * 2
    near, far, across = ([hop * PLANE + own for own in range(PLANE)] for hop in range(1, PLANES))
    own = ascending[: PLANE - 1]
    there = (near + far + across + own, far + across + near + own)
    near, far, across = near[::-1], far[::-1], across[::-1]
    back = (across + near + far + own, near + far + across + own)
    return there, back


def kernel(
    n, chunks, x_any, guard_any, train_any, high_any, low_any, cos_any, sin_any,
    power_ref, total_ref, scale_ref, band_ref, near_ref,
    sent, got, mixed, cells, landed, halo_out, halo_in, edges,
    x_ref, guard_ref, train_ref, table_high, table_low, twist_cos, twist_sin,
    send_one, recv_one, send_two, recv_two, send_halo, recv_halo, send_edge, recv_edge,
    load, row_in, last_in, higher, lower, row_known,
):
    me = lax.axis_index("pulse")
    length, gates = x_ref.shape[1], x_ref.shape[2]
    wide = gates // chunks
    part = wide // n
    halves = length // LANES
    groups = part // ROWS
    barrier = pltpu.get_barrier_semaphore()
    tiles = wide // LANES
    loads = []
    for t in range(chunks * tiles):
        lanes = slice(t * LANES, (t + 1) * LANES)
        loads.append((x_any.at[:, :, lanes], x_ref.at[:, :, lanes]))
    loads += [
        (guard_any, guard_ref), (train_any, train_ref), (cos_any, twist_cos),
        (sin_any, twist_sin), (high_any, table_high), (low_any, table_low),
    ]
    loads = [pltpu.make_async_copy(*pair, load.at[i]) for i, pair in enumerate(loads)]
    for copy in loads:
        copy.start()
    planes = n // PLANE
    last_plane = planes - 1
    plane, place = lax.div(me, PLANE), lax.rem(me, PLANE)
    row, core = lax.div(place, CORES), lax.rem(place, CORES)

    def chip(target, other):
        return target * PLANE + (row + other - 2 * other * row) * CORES

    def tell(semaphore, target, other):
        for k in range(CORES):
            peer = chip(target, other) + k
            pl.semaphore_signal(semaphore, inc=1, device_id={"pulse": peer})

    def hear(semaphore):
        pl.semaphore_wait(semaphore, CORES)

    pl.semaphore_signal(barrier, inc=1, device_id={"pulse": partner(me, 1)})

    @pl.when(plane < last_plane)
    def _():
        tell(barrier, plane + 1, 0)

    @pl.when((plane >= 1) & (plane < last_plane))
    def _():
        tell(barrier, plane - 1, 0)

    @pl.when(row == 0)
    def _():
        tell(barrier, plane, 1)

    def fill(t):
        loads[t].wait()
        c, first = t // tiles, t % tiles * LANES
        for p in range(2):
            block = x_ref[p, :, t * LANES : (t + 1) * LANES].T
            for d in range(first // part, -(-(first + LANES) // part)):
                begin, end = max(first, d * part), min(first + LANES, (d + 1) * part)
                sent[c, d, p, begin - d * part : end - d * part] = block[begin - first : end - first]

    inner = inner_flag(me, n)
    peers, back = (
        [
            (a + inner * (b - a), (1 - inner) * partner(me, a) + inner * partner(me, b))
            if a != b else (a, partner(me, a))
            for a, b in zip(*orders)
        ]
        for orders in peer_orders(n)
    )

    def first_copy(c, peer, source=me):
        return pltpu.make_async_remote_copy(
            src_ref=sent.at[c, peer], dst_ref=got.at[c, source],
            send_sem=send_one.at[c, peer], recv_sem=recv_one.at[c, source],
            device_id={"pulse": peer},
        )

    def second_copy(c, peer, source=me):
        rows = pl.ds(pl.multiple_of(source * part, ROWS), part)
        return pltpu.make_async_remote_copy(
            src_ref=cells.at[c, peer], dst_ref=landed.at[c, rows],
            send_sem=send_two.at[c], recv_sem=recv_two.at[c, source],
            device_id={"pulse": peer},
        )

    def halo_copy(peer):
        return pltpu.make_async_remote_copy(
            src_ref=halo_out.at[peer], dst_ref=halo_in.at[me],
            send_sem=send_halo, recv_sem=recv_halo,
            device_id={"pulse": peer},
        )

    def all_halos():
        others = pl.ds(0, n - 1)
        return pltpu.make_async_remote_copy(
            src_ref=halo_out.at[others], dst_ref=halo_in.at[others],
            send_sem=send_halo, recv_sem=recv_halo, device_id={"pulse": partner(me, 1)},
        )

    def all_sent(c):
        others = cells.at[c, pl.ds(0, n - 1)]
        return pltpu.make_async_remote_copy(
            src_ref=others, dst_ref=others,
            send_sem=send_two.at[c], recv_sem=recv_two.at[c, 0],
            device_id={"pulse": partner(me, 1)},
        )

    def send(target, other):
        for k in range(CORES):
            first_copy(0, chip(target, other) + partner(core, k)).start()

    for t in range(tiles):
        fill(t)

    beneath = lax.div(plane + last_plane, planes)
    above = 1 - lax.div(plane + 2, planes) if planes > 2 else 0
    pl.semaphore_wait(barrier, 1 + CORES * (beneath + above + row))

    @pl.when(row == 1)
    def _():
        tell(row_in, plane, 1)

    @pl.when((plane == last_plane) & (plane >= 1))
    def _():
        tell(last_in, plane - 1, 0)

    @pl.when((plane >= 1) & (plane + 1 < last_plane))
    def _():
        tell(higher.at[2], plane - 1, 0)
        tell(lower.at[2], plane + 1, 0)

    @pl.when(plane + 1 < last_plane)
    def _():
        send(plane + 1, 0)

    @pl.when(plane >= 1)
    def _():
        send(plane - 1, 0)

    first_copy(0, partner(me, 1)).start()

    @pl.when((plane >= 2) & (plane < last_plane))
    def _():
        hear(lower.at[2])
        send(plane - 2, 0)

    @pl.when(plane == last_plane - 1)
    def _():
        hear(last_in)

        @pl.when(plane >= 1)
        def _():
            tell(higher.at[2], plane - 1, 0)
            tell(lower.at[2], plane + 1, 0)

        send(plane + 1, 0)

    @pl.when(row == 0)
    def _():
        hear(row_in)

    tell(row_known.at[1], plane, 1)
    hear(row_known.at[1])
    send(plane, 1)
    for hop in (1, -1):
        @pl.when((plane + hop >= 0) & (plane + hop <= last_plane))
        def _():
            send(plane + hop, 1)

    for k in range(2, planes):
        @pl.when(plane + k <= last_plane)
        def _():
            hear(higher.at[k])

        @pl.when((plane >= k) if k > 2 else (plane == last_plane))
        def _():
            hear(lower.at[k])

        if k + 1 < planes:
            @pl.when((plane + k <= last_plane) & (plane >= 1))
            def _():
                tell(higher.at[k + 1], plane - 1, 0)

            @pl.when((plane >= k) & (plane < last_plane))
            def _():
                tell(lower.at[k + 1], plane + 1, 0)

        tell(row_known.at[k], plane, 1)
        @pl.when(plane + k <= last_plane)
        def _():
            send(plane + k, 0)

        @pl.when((plane >= k) if k > 2 else (plane == last_plane))
        def _():
            send(plane - k, 0)

        hear(row_known.at[k])
        for hop in (k, -k):
            @pl.when((plane + hop >= 0) & (plane + hop <= last_plane))
            def _():
                send(plane + hop, 1)

    for c in range(1, chunks):
        for t in range(c * tiles, (c + 1) * tiles):
            fill(t)
        for o, peer in peers:
            first_copy(c, peer).start()
    for c in range(chunks):
        got[c, me] = sent[c, me]
    for copy in loads[chunks * tiles :]:
        copy.wait()
    guard, train = guard_ref[0], train_ref[0]
    taps = lax.broadcasted_iota(jnp.int32, band_ref.shape, 0) - LANES
    taps = jnp.abs(taps - lax.broadcasted_iota(jnp.int32, band_ref.shape, 1))
    inside = (taps > guard) & (taps <= guard + train)
    band_ref[...] = inside.astype(jnp.float32).astype(jnp.bfloat16)
    gate = lax.broadcasted_iota(jnp.int32, scale_ref.shape, 1)
    before = jnp.minimum(jnp.maximum(gate - guard, 0), train)
    after = jnp.minimum(jnp.maximum(gates - 1 - gate - guard, 0), train)
    scale_ref[...] = (before + after).astype(jnp.float32) + 2.0 * TRAIN_BINS
    bins = lax.broadcasted_iota(jnp.int32, (length, length), 0)
    bins = jnp.abs(bins - lax.broadcasted_iota(jnp.int32, (length, length), 1))
    inside = (bins > GUARD_BINS) & (bins <= GUARD_BINS + TRAIN_BINS)
    near_ref[...] = inside.astype(jnp.float32).astype(jnp.bfloat16)

    def spectra(c):
        for r in range(0, part, ROWS):
            for h in range(halves):
                lanes = slice(h * LANES, (h + 1) * LANES)
                spectrum = butterflies(
                    [
                        (got[c, s, 0, r : r + ROWS, lanes], got[c, s, 1, r : r + ROWS, lanes])
                        for s in range(n)
                    ]
                )
                for f, (re, im) in enumerate(spectrum):
                    tc, ts = twist_cos[f : f + 1, lanes], twist_sin[f : f + 1, lanes]
                    mixed[0, f, r : r + ROWS, lanes] = tc * re + ts * im
                    mixed[1, f, r : r + ROWS, lanes] = tc * im - ts * re
        high, low = split(mixed[...].reshape(2 * n * part, length))
        both = (
            bf16_dot(high, table_high[...])
            + bf16_dot(low, table_high[...])
            + bf16_dot(high, table_low[...])
        ).reshape(2, n * part, 2 * length)
        real = both[0, :, :length] + both[1, :, length:]
        imag = both[1, :, :length] - both[0, :, length:]
        power = (real * real + imag * imag).reshape(n, part, length)
        rows = [
            [power[f, :, h * LANES : (h + 1) * LANES] for h in range(halves)] for f in range(n)
        ]
        rows = swap_digits(rows, 1)
        for d in range(n):
            for h in range(halves):
                cells[c, d, :, h * LANES : (h + 1) * LANES] = rows[d][h]
        if c < chunks - 1:
            return
        lane = lax.broadcasted_iota(jnp.int32, (part, LANES), 1)
        for d in range(n):
            ends = jnp.where(
                lane >= LANES - ROWS, rows[(d + n - 1) % n][halves - 1],
                jnp.where(lane < ROWS, rows[(d + 1) % n][0], 0.0),
            )
            ends = pltpu.roll(ends, ROWS, 1, stride=2 * ROWS, stride_axis=0)
            halo_out[d] = jnp.sum(ends.reshape(groups, ROWS, LANES), axis=1)

    for c in range(chunks):
        for o, peer in peers:
            first_copy(c, peer, peer).wait_recv()
        spectra(c)
        for o, peer in back:
            if c == chunks - 1:
                halo_copy(peer).start()
            second_copy(c, peer).start()
        landed[c, pl.ds(pl.multiple_of(me * part, ROWS), part)] = cells[c, me]
    halo_in[me] = halo_out[me]

    def edge_copies(c):
        ends = ((length - ROWS, 0, 1), (0, 1, n - 1))
        return [
            pltpu.make_async_remote_copy(
                src_ref=power_ref.at[row : row + ROWS, c * wide : (c + 1) * wide],
                dst_ref=edges.at[c, side],
                send_sem=send_edge.at[c, side], recv_sem=recv_edge.at[c, side],
                device_id={"pulse": lax.rem(me + hop, n)},
            )
            for row, side, hop in ends
        ]

    upper = lax.div(2 * me, n)

    def arrive(c):
        below = 0
        for k in range(tiles):
            covered = -(-(k + 1) * LANES // part)
            for d in range(below, covered):
                peer = d + upper * (n - 1 - 2 * d)

                @pl.when(peer != me)
                def _():
                    second_copy(c, peer, peer).wait_recv()

            below = covered
            first = (k + upper * (tiles - 1 - 2 * k)) * LANES
            rows = pl.ds(pl.multiple_of(first, LANES), LANES)
            columns = pl.ds(pl.multiple_of(c * wide + first, LANES), LANES)
            power_ref[:, columns] = landed[c, rows].T

    rest = jnp.zeros((ROWS, wide), jnp.float32)

    def add_edges(columns, before, after):
        head, tail = jnp.concatenate([before, rest]), jnp.concatenate([rest, after])
        top, bottom = total_ref[:ROWS, columns], total_ref[length - ROWS :, columns]
        for d in range(GUARD_BINS + 1, GUARD_BINS + TRAIN_BINS + 1):
            top = top + head[ROWS - d : 2 * ROWS - d]
            bottom = bottom + tail[d : d + ROWS]
        total_ref[:ROWS, columns] = top
        total_ref[length - ROWS :, columns] = bottom

    final = gates - wide
    for c in range(chunks - 1):
        arrive(c)
        for copy in edge_copies(c):
            copy.start()
    total_ref[:, :final] = scale_ref[:1, :final] + near_sum(near_ref, power_ref[:, :final])
    total_ref[:, final:] = jnp.broadcast_to(scale_ref[:1, final:], (length, wide))
    for first in range(0, gates, BLOCK):
        last, begin = min(first + BLOCK, gates), max(0, first - LANES)
        end = min(final, last + LANES)
        if begin < end:
            total_ref[:, first:last] += band_sum(band_ref, power_ref, first, last, begin, end)
    for c in range(chunks - 1):
        for copy in edge_copies(c):
            copy.wait_recv()
        add_edges(slice(c * wide, (c + 1) * wide), edges[c, 0], edges[c, 1])
    for first in range(0, gates, BLOCK):
        if complete(first, gates, final):
            own = slice(first, min(first + BLOCK, gates))
            total_ref[:, own] = power_ref[:, own] * scale_ref[:1, own] / total_ref[:, own]
    for c in range(chunks):
        for o, peer in peers:
            first_copy(c, peer).wait_send()
        if c < chunks - 1:
            all_sent(c).wait_send()
    for c in range(chunks - 1):
        for copy in edge_copies(c):
            copy.wait_send()
    all_halos().wait_recv()
    gate_row = lax.broadcasted_iota(jnp.int32, (wide, LANES), 0)
    lane = lax.broadcasted_iota(jnp.int32, (wide, LANES), 1)
    packed = halo_in[...].reshape(n * groups, 1, LANES)
    packed = jnp.broadcast_to(packed, (n * groups, ROWS, LANES)).reshape(wide, LANES)
    high, low = split(jnp.where(lane // (2 * ROWS) == gate_row % ROWS, packed, 0.0))
    slot = lax.broadcasted_iota(jnp.int32, (2 * ROWS, LANES), 0)
    lane = lax.broadcasted_iota(jnp.int32, (2 * ROWS, LANES), 1)
    fold = (lane % (2 * ROWS) == slot).astype(jnp.float32).astype(jnp.bfloat16)
    last_dims = (((1,), (1,)), ((), ()))
    halos = bf16_dot(fold, high, last_dims) + bf16_dot(fold, low, last_dims)
    add_edges(slice(final, gates), halos[:ROWS], halos[ROWS:])
    arrive(chunks - 1)
    all_halos().wait_send()
    all_sent(chunks - 1).wait_send()


def complete(first, gates, final):
    return min(gates, first + BLOCK + LANES) <= final


def near_sum(near_ref, powers):
    high, low = split(powers)
    return bf16_dot(near_ref[...], high) + bf16_dot(near_ref[...], low)


def band_sum(band_ref, power_ref, first, last, begin, end):
    high, low = split(power_ref[:, begin:end])
    band = band_ref[begin - first + LANES : end - first + LANES, : last - first]
    return bf16_dot(high, band) + bf16_dot(low, band)


def tables(n, length):
    lane = np.arange(length)
    width = length // n
    bins = width * (lane % n) + lane // n
    turn = 2 * np.pi * (np.outer(lane, bins) % length) / length
    both = np.concatenate([np.cos(turn), np.sin(turn)], axis=1).astype(np.float32)
    high = both.astype(jnp.bfloat16)
    low = (both - high.astype(np.float32)).astype(jnp.bfloat16)
    twist = 2 * np.pi * np.outer(np.arange(n), lane) / (n * length)
    scale = 1.0 / np.sqrt(n * length)
    return (
        high, low,
        (np.cos(twist) * scale).astype(np.float32),
        (np.sin(twist) * scale).astype(np.float32),
    )


def kernel_shards(echoes, guard_gates, train_gates):
    n = lax.axis_size("pulse")
    length, gates = echoes.shape[1], echoes.shape[2]
    chunks = CHUNKS
    part = gates // n // chunks
    wide = n * part
    groups = part // ROWS
    vmem = pl.BlockSpec(memory_space=pltpu.VMEM)
    out = jax.ShapeDtypeStruct((length, gates), jnp.float32)
    dma = pltpu.SemaphoreType.DMA
    constants = tuple(jnp.asarray(t) for t in tables(n, length))
    echoes, *constants = (
        pltpu.with_memory_space_constraint(t, pltpu.HBM) for t in (echoes, *constants)
    )
    operands = (echoes, guard_gates, train_gates, *constants)
    results = pl.pallas_call(
        functools.partial(kernel, n, chunks),
        out_shape=(
            out, out, jax.ShapeDtypeStruct((ROWS, gates), jnp.float32),
            jax.ShapeDtypeStruct((BLOCK + 2 * LANES, BLOCK), jnp.bfloat16),
            jax.ShapeDtypeStruct((length, length), jnp.bfloat16),
        ),
        in_specs=[pl.BlockSpec(memory_space=pl.ANY)] * len(operands),
        out_specs=(vmem,) * 5,
        scratch_shapes=[
            pltpu.VMEM((chunks, n, 2, part, length), jnp.float32),
            pltpu.VMEM((chunks, n, 2, part, length), jnp.float32),
            pltpu.VMEM((2, n, part, length), jnp.float32),
            pltpu.VMEM((chunks, n, part, length), jnp.float32),
            pltpu.VMEM((chunks, wide, length), jnp.float32),
            pltpu.VMEM((n, groups, LANES), jnp.float32),
            pltpu.VMEM((n, groups, LANES), jnp.float32),
            pltpu.VMEM((chunks - 1, 2, ROWS, wide), jnp.float32),
            pltpu.VMEM(echoes.shape, jnp.float32),
            pltpu.SMEM((1,), jnp.int32),
            pltpu.SMEM((1,), jnp.int32),
            pltpu.VMEM((length, 2 * length), jnp.bfloat16),
            pltpu.VMEM((length, 2 * length), jnp.bfloat16),
            pltpu.VMEM((n, length), jnp.float32),
            pltpu.VMEM((n, length), jnp.float32),
            *[dma((chunks, n))] * 2, dma((chunks,)), dma((chunks, n)), dma, dma,
            dma((chunks - 1, 2)), dma((chunks - 1, 2)), dma((gates // LANES + 6,)),
            pltpu.SemaphoreType.REGULAR, pltpu.SemaphoreType.REGULAR,
            *[pltpu.SemaphoreType.REGULAR((max(3, n // PLANE),))] * 3,
        ],
        compiler_params=pltpu.CompilerParams(
            collective_id=0, has_side_effects=True, vmem_limit_bytes=24 * 2**20
        ),
        cost_estimate=pl.CostEstimate(
            flops=KERNEL_FLOPS, bytes_accessed=2 * 4 * length * gates, transcendentals=0
        ),
    )(*operands)
    return pl.pallas_call(
        functools.partial(write_out, gates - wide),
        out_shape=(out, out),
        in_specs=[vmem] * 5,
        out_specs=(pl.BlockSpec(memory_space=pl.ANY),) * 2,
        scratch_shapes=[pltpu.VMEM((length, gates), jnp.float32), dma((1 + gates // BLOCK,))],
        compiler_params=pltpu.CompilerParams(vmem_limit_bytes=12 * 2**20),
    )(*results)


def write_out(
    final, power_ref, total_ref, scale_ref, band_ref, near_ref, power_out, stat_out, stat_ref, done
):
    gates = power_ref.shape[1]
    copies = []

    def put(source, target):
        copies.append(pltpu.make_async_copy(source, target, done.at[len(copies)]))
        copies[-1].start()

    put(power_ref, power_out)
    for first in range(0, gates, BLOCK):
        own = slice(first, min(first + BLOCK, gates))
        if complete(first, gates, final):
            put(total_ref.at[:, own], stat_out.at[:, own])
    for first in range(0, gates, BLOCK):
        if complete(first, gates, final):
            continue
        last = min(first + BLOCK, gates)
        begin, end = max(final, first - LANES), min(gates, last + LANES)
        total = total_ref[:, first:last]
        total = total + band_sum(band_ref, power_ref, first, last, begin, end)
        late = max(first, final)
        near = near_sum(near_ref, power_ref[:, late:last])
        if late > first:
            near = jnp.concatenate([jnp.zeros_like(power_ref[:, first:late]), near], axis=1)
        own = slice(first, last)
        stat_ref[:, own] = power_ref[:, own] * scale_ref[:1, own] / (total + near)
        put(stat_ref.at[:, own], stat_out.at[:, own])
    for copy in copies:
        copy.wait()


CHUNKS = 2
BLOCK = 256
KERNEL_FLOPS = 10**10
PLANE = 4
CORES = 2
PLANES = 4
REACH = 20


def shards(echoes, guard_gates, train_gates):
    n = lax.axis_size("pulse")
    length, gates = echoes.shape[1], echoes.shape[2]
    fits = length % LANES == 0 and length % n == 0 and n % PLANE == 0 and n <= LANES
    fits = fits and gates % (n * ROWS * CHUNKS) == 0 and gates % (LANES * CHUNKS) == 0
    fits = fits and n & (n - 1) == 0 and length & (length - 1) == 0 and REACH <= LANES
    if fits and GUARD_BINS + TRAIN_BINS <= ROWS:
        return kernel_shards(echoes, guard_gates, train_gates)
    return generic_shards(echoes, guard_gates, train_gates)


def solution(mesh):
    return jax.shard_map(
        shards,
        mesh=mesh,
        in_specs=(P(None, "pulse", "beam"), P(), P()),
        out_specs=(P("pulse", "beam"), P("pulse", "beam")),
        check_vma=False,
    )
```

```python
import functools

import jax
import jax.numpy as jnp
import numpy as np
from jax import lax
from jax.experimental import pallas as pl
from jax.experimental.pallas import tpu as pltpu
from jax.sharding import PartitionSpec as P

PULSES = 4096
GUARD_BINS = 2
TRAIN_BINS = 4


TWO_PI = 6.283185307179586


def padded_2(cells, sides, width):
    for axis, dim in sides:
        count = lax.axis_size(axis)
        head = lax.slice_in_dim(cells, 0, width, axis=dim)
        tail = lax.slice_in_dim(cells, cells.shape[dim] - width, cells.shape[dim], axis=dim)
        cells = jnp.concatenate(
            [
                lax.ppermute(tail, axis, [(i, (i + 1) % count) for i in range(count)]),
                cells,
                lax.ppermute(head, axis, [((i + 1) % count, i) for i in range(count)]),
            ],
            axis=dim,
        )
    return cells


def small_tables(count):
    index_row = jnp.arange(count, dtype=jnp.int32)
    phases = (index_row[:, None] * index_row[None, :] % count).astype(jnp.float32) * (
        TWO_PI / count
    )
    return (jnp.cos(phases), jnp.sin(phases))


def product(left, right):
    return jnp.dot(left, right, precision=lax.Precision.HIGHEST, preferred_element_type=jnp.float32)


def factored_powers(samples):
    width = samples.shape[2]
    bit_count = PULSES.bit_length() - 1
    first_radix = 2 ** (bit_count // 2)
    second_radix = PULSES // first_radix
    cos_first, sin_first = small_tables(first_radix)
    real_in = samples[0].reshape(first_radix, second_radix * width)
    imag_in = samples[1].reshape(first_radix, second_radix * width)
    real_one = (product(cos_first, real_in) + product(sin_first, imag_in)).reshape(
        first_radix, second_radix, width
    )
    imag_one = (product(cos_first, imag_in) - product(sin_first, real_in)).reshape(
        first_radix, second_radix, width
    )
    first_ids = jnp.arange(first_radix, dtype=jnp.int32)
    second_ids = jnp.arange(second_radix, dtype=jnp.int32)
    twist = (first_ids[:, None] * second_ids[None, :] % PULSES).astype(jnp.float32) * (
        TWO_PI / PULSES
    )
    twist_cos = jnp.cos(twist)[:, :, None]
    twist_sin = jnp.sin(twist)[:, :, None]
    real_two = twist_cos * real_one + twist_sin * imag_one
    imag_two = twist_cos * imag_one - twist_sin * real_one
    real_two = jnp.transpose(real_two, (1, 0, 2)).reshape(second_radix, first_radix * width)
    imag_two = jnp.transpose(imag_two, (1, 0, 2)).reshape(second_radix, first_radix * width)
    cos_second, sin_second = small_tables(second_radix)
    scale_factor = 1.0 / jnp.sqrt(jnp.float32(PULSES))
    real_out = (product(cos_second, real_two) + product(sin_second, imag_two)) * scale_factor
    imag_out = (product(cos_second, imag_two) - product(sin_second, real_two)) * scale_factor
    result = real_out * real_out + imag_out * imag_out
    return result.reshape(PULSES, width)


def generic_shards(echoes, guard_gates, train_gates):
    devices_count = lax.axis_size("pulse")
    bins_local = PULSES // devices_count
    gates_count = echoes.shape[2]
    columns = factored_powers(
        lax.all_to_all(echoes, "pulse", split_axis=2, concat_axis=1, tiled=True)
    )
    powers = lax.all_to_all(columns, "pulse", split_axis=0, concat_axis=1, tiled=True)
    reach = GUARD_BINS + TRAIN_BINS
    padded = padded_2(powers, (("pulse", 0),), reach)
    doppler_sum = jnp.zeros_like(powers)
    for shift_bins in range(GUARD_BINS + 1, reach + 1):
        above = padded[reach + shift_bins : reach + shift_bins + bins_local]
        below = padded[reach - shift_bins : reach - shift_bins + bins_local]
        doppler_sum = doppler_sum + above + below
    guard_width = guard_gates[0]
    train_width = train_gates[0]
    gate_ids = jnp.arange(gates_count, dtype=jnp.int32)
    offsets = jnp.abs(gate_ids[:, None] - gate_ids[None, :])
    band = ((offsets > guard_width) & (offsets <= guard_width + train_width)).astype(jnp.float32)
    range_sum = jnp.dot(
        powers, band, precision=lax.Precision.HIGHEST, preferred_element_type=jnp.float32
    )
    range_count = jnp.sum(band, axis=0)
    noise_level = (range_sum + doppler_sum) / (range_count[None, :] + 2.0 * TRAIN_BINS)
    statistic = powers / (noise_level + 1.0)
    return (powers, statistic)


LANES = 128
ROWS = 8
HIGHEST = lax.Precision.HIGHEST


def butterflies(cells):
    count = len(cells)
    if count == 1:
        return cells
    even = butterflies(cells[0::2])
    odd = butterflies(cells[1::2])
    low, high = [], []
    for k in range(count // 2):
        re, im = odd[k]
        if 4 * k == count:
            re, im = im, -re
        elif k:
            c, s = np.cos(2 * np.pi * k / count), np.sin(2 * np.pi * k / count)
            c, s = np.float32(c), np.float32(s)
            re, im = c * re + s * im, c * im - s * re
        low.append((even[k][0] + re, even[k][1] + im))
        high.append((even[k][0] - re, even[k][1] - im))
    return low + high


def swap_digits(rows, width):
    count = len(rows)
    lane = lax.broadcasted_iota(jnp.int32, rows[0][0].shape, 1)
    bit = 1
    while bit < count:
        step = bit * width
        keep = (lane // step) % 2 == 0 if step < LANES else None
        for f in range(count):
            if f & bit:
                continue
            first, second = rows[f], rows[f | bit]
            if step < LANES:
                new_first = [
                    jnp.where(keep, a, pltpu.roll(b, step, 1)) for a, b in zip(first, second)
                ]
                new_second = [
                    jnp.where(keep, pltpu.roll(a, LANES - step, 1), b)
                    for a, b in zip(first, second)
                ]
            else:
                hop = step // LANES
                new_first, new_second = list(first), list(second)
                for h in range(len(first)):
                    if h & hop:
                        new_first[h] = second[h ^ hop]
                    else:
                        new_second[h] = first[h ^ hop]
            rows[f], rows[f | bit] = new_first, new_second
        bit *= 2
    return rows


def split(values):
    high = values.astype(jnp.bfloat16)
    return high, (values - high.astype(jnp.float32)).astype(jnp.bfloat16)


def bf16_dot(left, right, dims=(((1,), (0,)), ((), ()))):
    return lax.dot_general(left, right, dims, preferred_element_type=jnp.float32)


def inner_flag(me, n):
    plane = lax.div(me, PLANE)
    return lax.rem(lax.div(plane + 1, 2), 2)


def partner(me, offset):
    peer, bit = me, 1
    while bit <= offset:
        if offset & bit:
            peer = peer + bit * (1 - 2 * lax.rem(lax.div(me, bit), 2))
        bit *= 2
    return peer


def peer_orders(n):
    ascending = list(range(1, n))
    if n != PLANES * PLANE:
        return ((ascending, ascending),) * 2
    near, far, across = ([hop * PLANE + own for own in range(PLANE)] for hop in range(1, PLANES))
    own = ascending[: PLANE - 1]
    there = (near + far + across + own, far + across + near + own)
    near, far, across = near[::-1], far[::-1], across[::-1]
    back = (across + near + far + own, near + far + across + own)
    return there, back


def kernel(
    n, chunks, x_any, guard_any, train_any, high_any, low_any, cos_any, sin_any,
    power_ref, total_ref, scale_ref, band_ref, near_ref,
    sent, got, mixed, cells, landed, halo_out, halo_in, edges,
    x_ref, guard_ref, train_ref, table_high, table_low, twist_cos, twist_sin,
    send_one, recv_one, send_two, recv_two, send_halo, recv_halo, send_edge, recv_edge,
    load, row_in, last_in, higher, lower, row_known,
):
    me = lax.axis_index("pulse")
    length, gates = x_ref.shape[1], x_ref.shape[2]
    wide = gates // chunks
    part = wide // n
    halves = length // LANES
    groups = part // ROWS
    barrier = pltpu.get_barrier_semaphore()
    tiles = wide // LANES
    loads = []
    for t in range(chunks * tiles):
        lanes = slice(t * LANES, (t + 1) * LANES)
        loads.append((x_any.at[:, :, lanes], x_ref.at[:, :, lanes]))
    loads += [
        (guard_any, guard_ref), (train_any, train_ref), (cos_any, twist_cos),
        (sin_any, twist_sin), (high_any, table_high), (low_any, table_low),
    ]
    loads = [pltpu.make_async_copy(*pair, load.at[i]) for i, pair in enumerate(loads)]
    for copy in loads[:tiles]:
        copy.start()
    planes = n // PLANE
    last_plane = planes - 1
    plane, place = lax.div(me, PLANE), lax.rem(me, PLANE)
    row, core = lax.div(place, CORES), lax.rem(place, CORES)

    def chip(target, other):
        return target * PLANE + (row + other - 2 * other * row) * CORES

    def tell(semaphore, target, other):
        for k in range(CORES):
            peer = chip(target, other) + k
            pl.semaphore_signal(semaphore, inc=1, device_id={"pulse": peer})

    def hear(semaphore):
        pl.semaphore_wait(semaphore, CORES)

    pl.semaphore_signal(barrier, inc=1, device_id={"pulse": partner(me, 1)})

    @pl.when(plane < last_plane)
    def _():
        tell(barrier, plane + 1, 0)

    @pl.when((plane >= 1) & (plane < last_plane))
    def _():
        tell(barrier, plane - 1, 0)

    @pl.when(row == 0)
    def _():
        tell(barrier, plane, 1)

    def fill(t):
        loads[t].wait()
        c, first = t // tiles, t % tiles * LANES
        for p in range(2):
            block = x_ref[p, :, t * LANES : (t + 1) * LANES].T
            for d in range(first // part, -(-(first + LANES) // part)):
                begin, end = max(first, d * part), min(first + LANES, (d + 1) * part)
                sent[c, d, p, begin - d * part : end - d * part] = block[begin - first : end - first]

    inner = inner_flag(me, n)
    peers, back = (
        [
            (a + inner * (b - a), (1 - inner) * partner(me, a) + inner * partner(me, b))
            if a != b else (a, partner(me, a))
            for a, b in zip(*orders)
        ]
        for orders in peer_orders(n)
    )

    def first_copy(c, peer, source=me):
        return pltpu.make_async_remote_copy(
            src_ref=sent.at[c, peer], dst_ref=got.at[c, source],
            send_sem=send_one.at[c, peer], recv_sem=recv_one.at[c, source],
            device_id={"pulse": peer},
        )

    def second_copy(c, peer, source=me):
        rows = pl.ds(pl.multiple_of(source * part, ROWS), part)
        return pltpu.make_async_remote_copy(
            src_ref=cells.at[c, peer], dst_ref=landed.at[c, rows],
            send_sem=send_two.at[c], recv_sem=recv_two.at[c, source],
            device_id={"pulse": peer},
        )

    def halo_copy(peer):
        return pltpu.make_async_remote_copy(
            src_ref=halo_out.at[peer], dst_ref=halo_in.at[me],
            send_sem=send_halo, recv_sem=recv_halo,
            device_id={"pulse": peer},
        )

    def all_halos():
        others = pl.ds(0, n - 1)
        return pltpu.make_async_remote_copy(
            src_ref=halo_out.at[others], dst_ref=halo_in.at[others],
            send_sem=send_halo, recv_sem=recv_halo, device_id={"pulse": partner(me, 1)},
        )

    def all_sent(c):
        others = cells.at[c, pl.ds(0, n - 1)]
        return pltpu.make_async_remote_copy(
            src_ref=others, dst_ref=others,
            send_sem=send_two.at[c], recv_sem=recv_two.at[c, 0],
            device_id={"pulse": partner(me, 1)},
        )

    def send(target, other):
        for k in range(CORES):
            first_copy(0, chip(target, other) + partner(core, k)).start()

    for t in range(tiles):
        fill(t)
    for copy in loads[tiles:]:
        copy.start()

    beneath = lax.div(plane + last_plane, planes)
    above = 1 - lax.div(plane + 2, planes) if planes > 2 else 0
    pl.semaphore_wait(barrier, 1 + CORES * (beneath + above + row))

    @pl.when(row == 1)
    def _():
        tell(row_in, plane, 1)

    @pl.when((plane == last_plane) & (plane >= 1))
    def _():
        tell(last_in, plane - 1, 0)

    @pl.when((plane >= 1) & (plane + 1 < last_plane))
    def _():
        tell(higher.at[2], plane - 1, 0)
        tell(lower.at[2], plane + 1, 0)

    @pl.when(plane + 1 < last_plane)
    def _():
        send(plane + 1, 0)

    @pl.when(plane >= 1)
    def _():
        send(plane - 1, 0)

    first_copy(0, partner(me, 1)).start()

    @pl.when((plane >= 2) & (plane < last_plane))
    def _():
        hear(lower.at[2])
        send(plane - 2, 0)

    @pl.when(plane == last_plane - 1)
    def _():
        hear(last_in)

        @pl.when(plane >= 1)
        def _():
            tell(higher.at[2], plane - 1, 0)
            tell(lower.at[2], plane + 1, 0)

        send(plane + 1, 0)

    @pl.when(row == 0)
    def _():
        hear(row_in)

    tell(row_known.at[1], plane, 1)
    hear(row_known.at[1])
    for hop in (1, -1):
        @pl.when((plane + hop >= 0) & (plane + hop <= last_plane))
        def _():
            send(plane + hop, 1)

    send(plane, 1)
    for k in range(2, planes):
        @pl.when(plane + k <= last_plane)
        def _():
            hear(higher.at[k])

        @pl.when((plane >= k) if k > 2 else (plane == last_plane))
        def _():
            hear(lower.at[k])

        if k + 1 < planes:
            @pl.when((plane + k <= last_plane) & (plane >= 1))
            def _():
                tell(higher.at[k + 1], plane - 1, 0)

            @pl.when((plane >= k) & (plane < last_plane))
            def _():
                tell(lower.at[k + 1], plane + 1, 0)

        @pl.when(plane + k <= last_plane)
        def _():
            send(plane + k, 0)

        @pl.when((plane >= k) if k > 2 else (plane == last_plane))
        def _():
            send(plane - k, 0)

        tell(row_known.at[k], plane, 1)
        hear(row_known.at[k])
        for hop in (k, -k):
            @pl.when((plane + hop >= 0) & (plane + hop <= last_plane))
            def _():
                send(plane + hop, 1)

    for c in range(1, chunks):
        for t in range(c * tiles, (c + 1) * tiles):
            fill(t)
        for o, peer in peers:
            first_copy(c, peer).start()
    for c in range(chunks):
        got[c, me] = sent[c, me]
    for copy in loads[chunks * tiles :]:
        copy.wait()
    guard, train = guard_ref[0], train_ref[0]
    taps = lax.broadcasted_iota(jnp.int32, band_ref.shape, 0) - LANES
    taps = jnp.abs(taps - lax.broadcasted_iota(jnp.int32, band_ref.shape, 1))
    inside = (taps > guard) & (taps <= guard + train)
    band_ref[...] = inside.astype(jnp.float32).astype(jnp.bfloat16)
    gate = lax.broadcasted_iota(jnp.int32, scale_ref.shape, 1)
    before = jnp.minimum(jnp.maximum(gate - guard, 0), train)
    after = jnp.minimum(jnp.maximum(gates - 1 - gate - guard, 0), train)
    scale_ref[...] = (before + after).astype(jnp.float32) + 2.0 * TRAIN_BINS
    bins = lax.broadcasted_iota(jnp.int32, (length, length), 0)
    bins = jnp.abs(bins - lax.broadcasted_iota(jnp.int32, (length, length), 1))
    inside = (bins > GUARD_BINS) & (bins <= GUARD_BINS + TRAIN_BINS)
    near_ref[...] = inside.astype(jnp.float32).astype(jnp.bfloat16)

    def spectra(c):
        for r in range(0, part, ROWS):
            for h in range(halves):
                lanes = slice(h * LANES, (h + 1) * LANES)
                spectrum = butterflies(
                    [
                        (got[c, s, 0, r : r + ROWS, lanes], got[c, s, 1, r : r + ROWS, lanes])
                        for s in range(n)
                    ]
                )
                for f, (re, im) in enumerate(spectrum):
                    tc, ts = twist_cos[f : f + 1, lanes], twist_sin[f : f + 1, lanes]
                    mixed[0, f, r : r + ROWS, lanes] = tc * re + ts * im
                    mixed[1, f, r : r + ROWS, lanes] = tc * im - ts * re
        high, low = split(mixed[...].reshape(2 * n * part, length))
        both = (
            bf16_dot(high, table_high[...])
            + bf16_dot(low, table_high[...])
            + bf16_dot(high, table_low[...])
        ).reshape(2, n * part, 2 * length)
        real = both[0, :, :length] + both[1, :, length:]
        imag = both[1, :, :length] - both[0, :, length:]
        power = (real * real + imag * imag).reshape(n, part, length)
        rows = [
            [power[f, :, h * LANES : (h + 1) * LANES] for h in range(halves)] for f in range(n)
        ]
        rows = swap_digits(rows, 1)
        for d in range(n):
            for h in range(halves):
                cells[c, d, :, h * LANES : (h + 1) * LANES] = rows[d][h]
        if c < chunks - 1:
            return
        lane = lax.broadcasted_iota(jnp.int32, (part, LANES), 1)
        for d in range(n):
            ends = jnp.where(
                lane >= LANES - ROWS, rows[(d + n - 1) % n][halves - 1],
                jnp.where(lane < ROWS, rows[(d + 1) % n][0], 0.0),
            )
            ends = pltpu.roll(ends, ROWS, 1, stride=2 * ROWS, stride_axis=0)
            halo_out[d] = jnp.sum(ends.reshape(groups, ROWS, LANES), axis=1)

    for c in range(chunks):
        for o, peer in peers:
            first_copy(c, peer, peer).wait_recv()
        spectra(c)
        for o, peer in back:
            if c == chunks - 1:
                halo_copy(peer).start()
            second_copy(c, peer).start()
        landed[c, pl.ds(pl.multiple_of(me * part, ROWS), part)] = cells[c, me]
    halo_in[me] = halo_out[me]

    def edge_copies(c):
        ends = ((length - ROWS, 0, 1), (0, 1, n - 1))
        return [
            pltpu.make_async_remote_copy(
                src_ref=power_ref.at[row : row + ROWS, c * wide : (c + 1) * wide],
                dst_ref=edges.at[c, side],
                send_sem=send_edge.at[c, side], recv_sem=recv_edge.at[c, side],
                device_id={"pulse": lax.rem(me + hop, n)},
            )
            for row, side, hop in ends
        ]

    upper = lax.div(2 * me, n)

    def arrive(c):
        below = 0
        for k in range(tiles):
            covered = -(-(k + 1) * LANES // part)
            for d in range(below, covered):
                peer = d + upper * (n - 1 - 2 * d)

                @pl.when(peer != me)
                def _():
                    second_copy(c, peer, peer).wait_recv()

            below = covered
            first = (k + upper * (tiles - 1 - 2 * k)) * LANES
            rows = pl.ds(pl.multiple_of(first, LANES), LANES)
            columns = pl.ds(pl.multiple_of(c * wide + first, LANES), LANES)
            power_ref[:, columns] = landed[c, rows].T

    rest = jnp.zeros((ROWS, wide), jnp.float32)

    def add_edges(columns, before, after):
        head, tail = jnp.concatenate([before, rest]), jnp.concatenate([rest, after])
        top, bottom = total_ref[:ROWS, columns], total_ref[length - ROWS :, columns]
        for d in range(GUARD_BINS + 1, GUARD_BINS + TRAIN_BINS + 1):
            top = top + head[ROWS - d : 2 * ROWS - d]
            bottom = bottom + tail[d : d + ROWS]
        total_ref[:ROWS, columns] = top
        total_ref[length - ROWS :, columns] = bottom

    final = gates - wide
    for c in range(chunks - 1):
        arrive(c)
        for copy in edge_copies(c):
            copy.start()
    total_ref[:, :final] = scale_ref[:1, :final] + near_sum(near_ref, power_ref[:, :final])
    total_ref[:, final:] = jnp.broadcast_to(scale_ref[:1, final:], (length, wide))
    for first in range(0, gates, BLOCK):
        last, begin = min(first + BLOCK, gates), max(0, first - LANES)
        end = min(final, last + LANES)
        if begin < end:
            total_ref[:, first:last] += band_sum(band_ref, power_ref, first, last, begin, end)
    for c in range(chunks - 1):
        for copy in edge_copies(c):
            copy.wait_recv()
        add_edges(slice(c * wide, (c + 1) * wide), edges[c, 0], edges[c, 1])
    for first in range(0, gates, BLOCK):
        if complete(first, gates, final):
            own = slice(first, min(first + BLOCK, gates))
            total_ref[:, own] = power_ref[:, own] * scale_ref[:1, own] / total_ref[:, own]
    for c in range(chunks):
        for o, peer in peers:
            first_copy(c, peer).wait_send()
        if c < chunks - 1:
            all_sent(c).wait_send()
    for c in range(chunks - 1):
        for copy in edge_copies(c):
            copy.wait_send()
    all_halos().wait_recv()
    gate_row = lax.broadcasted_iota(jnp.int32, (wide, LANES), 0)
    lane = lax.broadcasted_iota(jnp.int32, (wide, LANES), 1)
    packed = halo_in[...].reshape(n * groups, 1, LANES)
    packed = jnp.broadcast_to(packed, (n * groups, ROWS, LANES)).reshape(wide, LANES)
    high, low = split(jnp.where(lane // (2 * ROWS) == gate_row % ROWS, packed, 0.0))
    slot = lax.broadcasted_iota(jnp.int32, (2 * ROWS, LANES), 0)
    lane = lax.broadcasted_iota(jnp.int32, (2 * ROWS, LANES), 1)
    fold = (lane % (2 * ROWS) == slot).astype(jnp.float32).astype(jnp.bfloat16)
    last_dims = (((1,), (1,)), ((), ()))
    halos = bf16_dot(fold, high, last_dims) + bf16_dot(fold, low, last_dims)
    add_edges(slice(final, gates), halos[:ROWS], halos[ROWS:])
    arrive(chunks - 1)
    all_halos().wait_send()
    all_sent(chunks - 1).wait_send()


def complete(first, gates, final):
    return min(gates, first + BLOCK + LANES) <= final


def near_sum(near_ref, powers):
    high, low = split(powers)
    return bf16_dot(near_ref[...], high) + bf16_dot(near_ref[...], low)


def band_sum(band_ref, power_ref, first, last, begin, end):
    high, low = split(power_ref[:, begin:end])
    band = band_ref[begin - first + LANES : end - first + LANES, : last - first]
    return bf16_dot(high, band) + bf16_dot(low, band)


def tables(n, length):
    lane = np.arange(length)
    width = length // n
    bins = width * (lane % n) + lane // n
    turn = 2 * np.pi * (np.outer(lane, bins) % length) / length
    both = np.concatenate([np.cos(turn), np.sin(turn)], axis=1).astype(np.float32)
    high = both.astype(jnp.bfloat16)
    low = (both - high.astype(np.float32)).astype(jnp.bfloat16)
    twist = 2 * np.pi * np.outer(np.arange(n), lane) / (n * length)
    scale = 1.0 / np.sqrt(n * length)
    return (
        high, low,
        (np.cos(twist) * scale).astype(np.float32),
        (np.sin(twist) * scale).astype(np.float32),
    )


def kernel_shards(echoes, guard_gates, train_gates):
    n = lax.axis_size("pulse")
    length, gates = echoes.shape[1], echoes.shape[2]
    chunks = CHUNKS
    part = gates // n // chunks
    wide = n * part
    groups = part // ROWS
    vmem = pl.BlockSpec(memory_space=pltpu.VMEM)
    out = jax.ShapeDtypeStruct((length, gates), jnp.float32)
    dma = pltpu.SemaphoreType.DMA
    constants = tuple(jnp.asarray(t) for t in tables(n, length))
    echoes, *constants = (
        pltpu.with_memory_space_constraint(t, pltpu.HBM) for t in (echoes, *constants)
    )
    operands = (echoes, guard_gates, train_gates, *constants)
    results = pl.pallas_call(
        functools.partial(kernel, n, chunks),
        out_shape=(
            out, out, jax.ShapeDtypeStruct((ROWS, gates), jnp.float32),
            jax.ShapeDtypeStruct((BLOCK + 2 * LANES, BLOCK), jnp.bfloat16),
            jax.ShapeDtypeStruct((length, length), jnp.bfloat16),
        ),
        in_specs=[pl.BlockSpec(memory_space=pl.ANY)] * len(operands),
        out_specs=(vmem,) * 5,
        scratch_shapes=[
            pltpu.VMEM((chunks, n, 2, part, length), jnp.float32),
            pltpu.VMEM((chunks, n, 2, part, length), jnp.float32),
            pltpu.VMEM((2, n, part, length), jnp.float32),
            pltpu.VMEM((chunks, n, part, length), jnp.float32),
            pltpu.VMEM((chunks, wide, length), jnp.float32),
            pltpu.VMEM((n, groups, LANES), jnp.float32),
            pltpu.VMEM((n, groups, LANES), jnp.float32),
            pltpu.VMEM((chunks - 1, 2, ROWS, wide), jnp.float32),
            pltpu.VMEM(echoes.shape, jnp.float32),
            pltpu.SMEM((1,), jnp.int32),
            pltpu.SMEM((1,), jnp.int32),
            pltpu.VMEM((length, 2 * length), jnp.bfloat16),
            pltpu.VMEM((length, 2 * length), jnp.bfloat16),
            pltpu.VMEM((n, length), jnp.float32),
            pltpu.VMEM((n, length), jnp.float32),
            *[dma((chunks, n))] * 2, dma((chunks,)), dma((chunks, n)), dma, dma,
            dma((chunks - 1, 2)), dma((chunks - 1, 2)), dma((gates // LANES + 6,)),
            pltpu.SemaphoreType.REGULAR, pltpu.SemaphoreType.REGULAR,
            *[pltpu.SemaphoreType.REGULAR((max(3, n // PLANE),))] * 3,
        ],
        compiler_params=pltpu.CompilerParams(
            collective_id=0, has_side_effects=True, vmem_limit_bytes=24 * 2**20
        ),
        cost_estimate=pl.CostEstimate(
            flops=KERNEL_FLOPS, bytes_accessed=2 * 4 * length * gates, transcendentals=0
        ),
    )(*operands)
    return pl.pallas_call(
        functools.partial(write_out, gates - wide),
        out_shape=(out, out),
        in_specs=[vmem] * 5,
        out_specs=(pl.BlockSpec(memory_space=pl.ANY),) * 2,
        scratch_shapes=[pltpu.VMEM((length, gates), jnp.float32), dma((1 + gates // BLOCK,))],
        compiler_params=pltpu.CompilerParams(vmem_limit_bytes=12 * 2**20),
    )(*results)


def write_out(
    final, power_ref, total_ref, scale_ref, band_ref, near_ref, power_out, stat_out, stat_ref, done
):
    gates = power_ref.shape[1]
    copies = []

    def put(source, target):
        copies.append(pltpu.make_async_copy(source, target, done.at[len(copies)]))
        copies[-1].start()

    put(power_ref, power_out)
    for first in range(0, gates, BLOCK):
        own = slice(first, min(first + BLOCK, gates))
        if complete(first, gates, final):
            put(total_ref.at[:, own], stat_out.at[:, own])
    for first in range(0, gates, BLOCK):
        if complete(first, gates, final):
            continue
        last = min(first + BLOCK, gates)
        begin, end = max(final, first - LANES), min(gates, last + LANES)
        total = total_ref[:, first:last]
        total = total + band_sum(band_ref, power_ref, first, last, begin, end)
        late = max(first, final)
        near = near_sum(near_ref, power_ref[:, late:last])
        if late > first:
            near = jnp.concatenate([jnp.zeros_like(power_ref[:, first:late]), near], axis=1)
        own = slice(first, last)
        stat_ref[:, own] = power_ref[:, own] * scale_ref[:1, own] / (total + near)
        put(stat_ref.at[:, own], stat_out.at[:, own])
    for copy in copies:
        copy.wait()


CHUNKS = 2
BLOCK = 256
KERNEL_FLOPS = 10**10
PLANE = 4
CORES = 2
PLANES = 4
REACH = 20


def shards(echoes, guard_gates, train_gates):
    n = lax.axis_size("pulse")
    length, gates = echoes.shape[1], echoes.shape[2]
    fits = length % LANES == 0 and length % n == 0 and n % PLANE == 0 and n <= LANES
    fits = fits and gates % (n * ROWS * CHUNKS) == 0 and gates % (LANES * CHUNKS) == 0
    fits = fits and n & (n - 1) == 0 and length & (length - 1) == 0 and REACH <= LANES
    if fits and GUARD_BINS + TRAIN_BINS <= ROWS:
        return kernel_shards(echoes, guard_gates, train_gates)
    return generic_shards(echoes, guard_gates, train_gates)


def solution(mesh):
    return jax.shard_map(
        shards,
        mesh=mesh,
        in_specs=(P(None, "pulse", "beam"), P(), P()),
        out_specs=(P("pulse", "beam"), P("pulse", "beam")),
        check_vma=False,
    )
```
